32 devices in a mesh: ep: 8 (over z, y), dp: 4 (over x, core).
Axes of the slice: x: 2, y: 2, z: 4, core: 2. Of those that a mesh axis runs over, the one named last changes fastest.
Arguments:
- hidden_in: bfloat16 [49152, 1024], P(('ep', 'dp'))
- topk_idx: int32 [49152, 8], P(('ep', 'dp'))
- grad_out: bfloat16 [49152, 1024], P(('ep', 'dp'))
- norm_gain: float32 [1024], replicated
- w_router: bfloat16 [1024, 32], replicated
- w_gate: bfloat16 [32, 1024, 512], P('ep')
- w_up: bfloat16 [32, 1024, 512], P('ep')
- w_down: bfloat16 [32, 512, 1024], P('ep')
Outputs:
- output 1: bfloat16 [49152, 1024], P(('ep', 'dp'))
- output 2: bfloat16 [49152, 1024], P(('ep', 'dp'))
- output 3: float32 [], replicated
- output 4: float32 [1024], replicated
- output 5: float32 [1024, 32], replicated
- output 6: bfloat16 [32, 1024, 512], P('ep')
- output 7: bfloat16 [32, 1024, 512], P('ep')
- output 8: bfloat16 [32, 512, 1024], P('ep')
All inputs are finite; a program needn't handle non-finite values.
Results may differ from the reference program's by a relative error of at most 0.0108758.
Values are sent between devices in bfloat16 or wider.
A program may use at most 1 GiB of HBM per device.

```python
import math
import jax
import jax.numpy as jnp
from jax import lax

D = 1024
FF = 512
EXPERTS = 32
TOP = 8
TOK = 1536
N_DEV = 32
TOK_TOTAL = TOK * N_DEV
CAPACITY = TOK * TOP // EXPERTS + TOK * TOP // (2 * EXPERTS)
ROWS_TOTAL = EXPERTS * N_DEV * CAPACITY
EPS = 1e-6
ALPHA = 0.001
AUX_GRAD = 0.25 * math.sqrt(D * EXPERTS)


def draw_routing(key):
    mean_load = TOK * TOP // EXPERTS
    quarter = mean_load // 4
    half_count = EXPERTS // 2
    key_pair, key_base, key_dev = jax.random.split(key, 3)
    pair_perm = jax.random.permutation(key_pair, EXPERTS)
    base_shift = jax.random.randint(key_base, (half_count,), 0, quarter + 1)
    positions = jnp.arange(TOK * TOP, dtype=jnp.int32)

    def one_block(dev_key):
        key_extra, key_order = jax.random.split(dev_key)
        extra_shift = jax.random.randint(key_extra, (half_count,), 0, quarter + 1)
        shift = (base_shift + extra_shift).at[0].set(2 * quarter)
        loads = jnp.zeros((EXPERTS,), jnp.int32)
        loads = loads.at[pair_perm[0::2]].set(mean_load + shift)
        loads = loads.at[pair_perm[1::2]].set(mean_load - shift)
        ends = jnp.cumsum(loads)
        expert_of = jnp.sum((positions[:, None] >= ends[None, :]).astype(jnp.int32), axis=1)
        table = expert_of.reshape(TOP, TOK).T
        order = jax.random.permutation(key_order, TOK)
        return table[order]

    blocks = jax.vmap(one_block)(jax.random.split(key_dev, N_DEV))
    return blocks.reshape(TOK_TOTAL, TOP).astype(jnp.int32)


def setup_inputs(seed: int = 0) -> dict:
    keys = jax.random.split(jax.random.key(seed), 8)
    hidden_in = (0.25 * jax.random.normal(keys[0], (TOK_TOTAL, D), jnp.float32)).astype(jnp.bfloat16)
    topk_idx = draw_routing(keys[1])
    grad_out = jax.random.normal(keys[2], (TOK_TOTAL, D), jnp.float32).astype(jnp.bfloat16)
    norm_gain = jax.random.uniform(keys[3], (D,), jnp.float32, 0.5, 1.5)
    w_router = (jax.random.normal(keys[4], (D, EXPERTS), jnp.float32) / math.sqrt(D)).astype(jnp.bfloat16)
    w_gate = (jax.random.normal(keys[5], (EXPERTS, D, FF), jnp.float32) / math.sqrt(D)).astype(jnp.bfloat16)
    w_up = (jax.random.normal(keys[6], (EXPERTS, D, FF), jnp.float32) / math.sqrt(D)).astype(jnp.bfloat16)
    w_down = (jax.random.normal(keys[7], (EXPERTS, FF, D), jnp.float32) / math.sqrt(FF)).astype(jnp.bfloat16)
    return {'hidden_in': hidden_in, 'topk_idx': topk_idx, 'grad_out': grad_out, 'norm_gain': norm_gain, 'w_router': w_router, 'w_gate': w_gate, 'w_up': w_up, 'w_down': w_down}


def reference(hidden_in, topk_idx, grad_out, norm_gain, w_router, w_gate, w_up, w_down):
    x_f = hidden_in.astype(jnp.float32)
    inv_rms = lax.rsqrt(jnp.mean(x_f * x_f, axis=-1, keepdims=True) + EPS)
    normed = (x_f * inv_rms * norm_gain).astype(jnp.bfloat16)
    logits = jnp.dot(normed, w_router, preferred_element_type=jnp.float32)
    probs = jax.nn.softmax(logits, axis=-1)
    chosen = jnp.take_along_axis(probs, topk_idx, axis=1)
    chosen_sum = jnp.sum(chosen, axis=1, keepdims=True)
    weights = chosen / chosen_sum

    pick = (topk_idx[:, :, None] == jnp.arange(EXPERTS, dtype=jnp.int32)[None, None, :]).astype(jnp.int32)
    pick_dev = pick.reshape(N_DEV, TOK * TOP, EXPERTS)
    rank = jnp.sum((jnp.cumsum(pick_dev, axis=1) - pick_dev) * pick_dev, axis=2)
    dev_ids = jnp.arange(N_DEV, dtype=jnp.int32)[:, None]
    slot = ((topk_idx.reshape(N_DEV, TOK * TOP) * N_DEV + dev_ids) * CAPACITY + rank).reshape(-1)
    owner_tok = jnp.arange(TOK_TOTAL * TOP, dtype=jnp.int32) // TOP
    slot_tok = jnp.full((ROWS_TOTAL,), TOK_TOTAL, jnp.int32).at[slot].set(owner_tok)
    slot_w = jnp.zeros((ROWS_TOTAL,), jnp.float32).at[slot].set(weights.reshape(-1))

    def one_expert(operands):
        gate_w, up_w, down_w, tok_sel, w_sel = operands
        rows = jnp.take(normed, tok_sel, axis=0, mode='fill', fill_value=0)
        gate_pre = jnp.dot(rows, gate_w, preferred_element_type=jnp.float32)
        up_pre = jnp.dot(rows, up_w, preferred_element_type=jnp.float32)
        sig_gate = jax.nn.sigmoid(gate_pre)
        act_gate = gate_pre * sig_gate
        hidden = (act_gate * up_pre).astype(jnp.bfloat16)
        out_rows = jnp.dot(hidden, down_w, preferred_element_type=jnp.float32).astype(jnp.bfloat16)
        dy_rows = jnp.take(grad_out, tok_sel, axis=0, mode='fill', fill_value=0)
        d_out_rows = (dy_rows.astype(jnp.float32) * w_sel[:, None]).astype(jnp.bfloat16)
        d_hidden = jnp.dot(d_out_rows, down_w.T, preferred_element_type=jnp.float32)
        d_gate = (d_hidden * up_pre * sig_gate * (1.0 + gate_pre * (1.0 - sig_gate))).astype(jnp.bfloat16)
        d_up = (d_hidden * act_gate).astype(jnp.bfloat16)
        d_rows = (jnp.dot(d_gate, gate_w.T, preferred_element_type=jnp.float32) + jnp.dot(d_up, up_w.T, preferred_element_type=jnp.float32)).astype(jnp.bfloat16)
        grad_gate = jnp.dot(rows.T, d_gate, preferred_element_type=jnp.float32).astype(jnp.bfloat16)
        grad_up = jnp.dot(rows.T, d_up, preferred_element_type=jnp.float32).astype(jnp.bfloat16)
        grad_down = jnp.dot(hidden.T, d_out_rows, preferred_element_type=jnp.float32).astype(jnp.bfloat16)
        return out_rows, d_rows, grad_gate, grad_up, grad_down

    out_rows, d_rows, grad_gate, grad_up, grad_down = lax.map(one_expert, (w_gate, w_up, w_down, slot_tok.reshape(EXPERTS, -1), slot_w.reshape(EXPERTS, -1)))
    combined = jnp.take(out_rows.reshape(ROWS_TOTAL, D), slot, axis=0).reshape(TOK_TOTAL, TOP, D).astype(jnp.float32)
    block_out = (x_f + jnp.sum(combined * weights[:, :, None], axis=1)).astype(jnp.bfloat16)

    load_frac = jnp.sum(pick, axis=(0, 1)).astype(jnp.float32) / (TOP * TOK_TOTAL)
    mean_prob = jnp.mean(probs, axis=0)
    aux_loss = ALPHA * EXPERTS * jnp.sum(load_frac * mean_prob)

    d_weight = jnp.sum(combined * grad_out.astype(jnp.float32)[:, None, :], axis=2)
    d_chosen = (d_weight - jnp.sum(weights * d_weight, axis=1, keepdims=True)) / chosen_sum
    d_prob = jnp.sum(pick.astype(jnp.float32) * d_chosen[:, :, None], axis=1) + AUX_GRAD * EXPERTS * load_frac[None, :]
    d_logit = probs * (d_prob - jnp.sum(probs * d_prob, axis=1, keepdims=True))
    d_logit_bf = d_logit.astype(jnp.bfloat16)
    grad_router = jnp.dot(normed.T, d_logit_bf, preferred_element_type=jnp.float32)
    d_choice = jnp.take(d_rows.reshape(ROWS_TOTAL, D), slot, axis=0).reshape(TOK_TOTAL, TOP, D)
    d_normed = jnp.sum(d_choice.astype(jnp.float32), axis=1) + jnp.dot(d_logit_bf, w_router.T, preferred_element_type=jnp.float32)
    grad_norm_gain = jnp.sum(d_normed * x_f * inv_rms, axis=0)
    d_scaled = d_normed * norm_gain
    inv_cube = inv_rms * inv_rms * inv_rms
    grad_in = (grad_out.astype(jnp.float32) + inv_rms * d_scaled - x_f * inv_cube * jnp.mean(d_scaled * x_f, axis=-1, keepdims=True)).astype(jnp.bfloat16)
    return (block_out, grad_in, aux_loss, grad_norm_gain, grad_router, grad_gate, grad_up, grad_down)
```

```python
import functools
import math
import jax
import jax.numpy as jnp
from jax import lax
from jax.experimental import pallas as pl
from jax.experimental.pallas import tpu as pltpu
from jax.sharding import Mesh, PartitionSpec as P

EPS = 1e-6
ALPHA = 0.001
AUX_SCALE = 0.25
BF = jnp.bfloat16
F32 = jnp.float32
CHUNK = 256
SEG = 128
TILE = 256
LANES = 128
ANY = pl.BlockSpec(memory_space=pl.ANY)


def dot(a, b, dims=((1,), (0,))):
    return lax.dot_general(a, b, (dims, ((), ())), preferred_element_type=F32)


def dispatch_kernel(first, last, experts, cnt, start, end, h_ref, dy_ref, rank_ref, w_ref, *refs):
    n_alias = 0 if first == 0 else 3
    hs, dys, wr, hbuf, dbuf, wbuf, hz, wz, hx, dx, wx, sem, xsem = refs[n_alias:]
    i = pl.program_id(0)
    c = i + first
    rows = lax.broadcasted_iota(jnp.int32, (SEG, CHUNK), 0)

    def copies(e, at):
        at = pl.multiple_of(at, 16)
        return (
            pltpu.make_async_copy(hbuf.at[e], hs.at[e, pl.ds(at, SEG)], sem.at[0, e]),
            pltpu.make_async_copy(dbuf.at[e], dys.at[e, pl.ds(at, SEG)], sem.at[1, e]),
            pltpu.make_async_copy(wbuf.at[e], wr.at[e, pl.ds(at, SEG)], sem.at[2, e]),
        )

    def select(e, base):
        same = rows + base == rank_ref[pl.ds(e, 1), :]
        pick = jnp.where(same, 1.0, 0.0).astype(BF)
        weight = jnp.sum(jnp.where(same, w_ref[pl.ds(e, 1), :], 0.0), axis=1, keepdims=True)
        return (
            dot(pick, h_ref[...]).astype(BF),
            dot(pick, dy_ref[...]).astype(BF),
            jnp.broadcast_to(weight, (SEG, LANES)),
        )

    def group(q, carry):
        for u in range(4):
            e = q * 4 + u
            h_rows, dy_rows, w_rows = select(e, 0)

            @pl.when(i > 0)
            def _():
                for cp in copies(e, 0):
                    cp.wait()

            hbuf[e] = h_rows
            dbuf[e] = dy_rows
            wbuf[e] = w_rows
            for cp in copies(e, start[c * experts + e]):
                cp.start()
        return carry

    lax.fori_loop(0, experts // 4, group, 0)

    def overflow(e, carry):
        @pl.when(cnt[c * experts + e] > SEG)
        def _():
            h_rows, dy_rows, w_rows = select(e, SEG)
            hx[...] = h_rows
            dx[...] = dy_rows
            wx[...] = w_rows
            at = pl.multiple_of(start[c * experts + e] + SEG, 16)
            extra = (
                pltpu.make_async_copy(hx, hs.at[e, pl.ds(at, SEG)], xsem.at[0]),
                pltpu.make_async_copy(dx, dys.at[e, pl.ds(at, SEG)], xsem.at[1]),
                pltpu.make_async_copy(wx, wr.at[e, pl.ds(at, SEG)], xsem.at[2]),
            )
            for cp in extra:
                cp.start()
            for cp in extra:
                cp.wait()
        return carry

    lax.fori_loop(0, experts, overflow, 0)

    @pl.when(i == pl.num_programs(0) - 1)
    def _():
        def drain(e, carry):
            for cp in copies(e, 0):
                cp.wait()
            return carry

        lax.fori_loop(0, experts, drain, 0)
        if last:
            hz[...] = jnp.zeros_like(hz)
            wz[...] = jnp.zeros_like(wz)

            def tail(e, carry):
                at = pl.multiple_of(end[e], 16)
                zero = (
                    pltpu.make_async_copy(hz, hs.at[e, pl.ds(at, TILE)], xsem.at[0]),
                    pltpu.make_async_copy(hz, dys.at[e, pl.ds(at, TILE)], xsem.at[1]),
                    pltpu.make_async_copy(wz, wr.at[e, pl.ds(at, TILE)], xsem.at[2]),
                )
                for cp in zero:
                    cp.start()
                for cp in zero:
                    cp.wait()
                return carry

            lax.fori_loop(0, experts, tail, 0)


def dispatch(first, last, tables, h, dy, rank_t, w_t, cap, prev=None):
    tok, dim = h.shape
    experts = rank_t.shape[0]
    n = tok // CHUNK
    shapes = (
        jax.ShapeDtypeStruct((experts, cap, dim), BF),
        jax.ShapeDtypeStruct((experts, cap, dim), BF),
        jax.ShapeDtypeStruct((experts, cap, LANES), F32),
    )
    prev = () if prev is None else prev
    return pl.pallas_call(
        functools.partial(dispatch_kernel, first, last, experts),
        out_shape=shapes,
        grid_spec=pltpu.PrefetchScalarGridSpec(
            num_scalar_prefetch=3,
            grid=(n,),
            in_specs=[
                pl.BlockSpec((CHUNK, dim), lambda i, *_: (i, 0)),
                pl.BlockSpec((CHUNK, dim), lambda i, *_: (i, 0)),
                pl.BlockSpec((experts, CHUNK), lambda i, *_: (0, i)),
                pl.BlockSpec((experts, CHUNK), lambda i, *_: (0, i)),
            ] + [ANY] * len(prev),
            out_specs=[ANY] * 3,
            scratch_shapes=[
                pltpu.VMEM((experts, SEG, dim), BF),
                pltpu.VMEM((experts, SEG, dim), BF),
                pltpu.VMEM((experts, SEG, LANES), F32),
                pltpu.VMEM((TILE, dim), BF),
                pltpu.VMEM((TILE, LANES), F32),
                pltpu.VMEM((SEG, dim), BF),
                pltpu.VMEM((SEG, dim), BF),
                pltpu.VMEM((SEG, LANES), F32),
                pltpu.SemaphoreType.DMA((3, experts)),
                pltpu.SemaphoreType.DMA((3,)),
            ],
        ),
        input_output_aliases={7 + k: k for k in range(len(prev))},
        compiler_params=pltpu.CompilerParams(
            dimension_semantics=("arbitrary",), vmem_limit_bytes=40 << 20
        ),
        cost_estimate=pl.CostEstimate(
            flops=4 * n * experts * SEG * CHUNK * dim, bytes_accessed=n * experts * SEG * dim * 4, transcendentals=0
        ),
        name=f"dispatch_{first}",
    )(*tables, h, dy, rank_t, w_t, *prev)


def expert_kernel(tiles, h_ref, dy_ref, wr_ref, w_ref, o_ref, dh_ref, dw_ref, gw_ref, acc_g, acc_u, acc_d):
    z, i = pl.program_id(0), pl.program_id(1)
    used = tiles[z]
    slices, _, depth, ff = w_ref.shape[1:]
    dim = slices * depth

    @pl.when(i == 0)
    def _():
        acc_g[...] = jnp.zeros_like(acc_g)
        acc_u[...] = jnp.zeros_like(acc_u)
        acc_d[...] = jnp.zeros_like(acc_d)

    @pl.when(i < used)
    def _():
        rows = h_ref[0]
        dy_rows = dy_ref[0]
        w_gate = w_ref[0, :, 0].reshape(dim, ff)
        w_up = w_ref[0, :, 1].reshape(dim, ff)
        w_down = w_ref[0, :, 2].reshape(dim, ff)
        gate_pre = dot(rows, w_gate)
        up_pre = dot(rows, w_up)
        sig = jax.nn.sigmoid(gate_pre)
        act = gate_pre * sig
        hidden = (act * up_pre).astype(BF)
        out = dot(hidden, w_down, ((1,), (1,))).astype(BF)
        o_ref[0] = out
        dy_f = dy_rows.astype(F32)
        d_weight = jnp.sum(dy_f * out.astype(F32), axis=1, keepdims=True)
        dw_ref[0] = jnp.broadcast_to(d_weight, dw_ref.shape[1:])
        d_out = (dy_f * wr_ref[0][:, :1]).astype(BF)
        d_hidden = dot(d_out, w_down)
        d_gate = (d_hidden * up_pre * sig * (1.0 + gate_pre * (1.0 - sig))).astype(BF)
        d_up = (d_hidden * act).astype(BF)
        dh_ref[0] = (dot(d_gate, w_gate, ((1,), (1,))) + dot(d_up, w_up, ((1,), (1,)))).astype(BF)
        acc_g[...] += dot(rows, d_gate, ((0,), (0,)))
        acc_u[...] += dot(rows, d_up, ((0,), (0,)))
        acc_d[...] += dot(d_out, hidden, ((0,), (0,)))

    @pl.when(i == used)
    def _():
        o_ref[...] = jnp.zeros_like(o_ref)
        dh_ref[...] = jnp.zeros_like(dh_ref)
        dw_ref[...] = jnp.zeros_like(dw_ref)

    @pl.when(i == pl.num_programs(1) - 1)
    def _():
        gw_ref[0, :, 0] = acc_g[...].astype(BF).reshape(slices, depth, ff)
        gw_ref[0, :, 1] = acc_u[...].astype(BF).reshape(slices, depth, ff)
        gw_ref[0, :, 2] = acc_d[...].astype(BF).reshape(slices, depth, ff)


def run_experts(j, n_local, tiles, hs, dys, wr, w):
    n_exp, cap, dim = hs.shape
    groups, slices, _, depth, ff = w.shape
    steps = cap // TILE

    def row_map(z, i, t):
        return (z * n_local + j, jnp.minimum(i, jnp.maximum(t[z] - 1, 0)), 0)

    def out_map(z, i, t):
        return (z, jnp.minimum(i, t[z]), 0)

    return pl.pallas_call(
        expert_kernel,
        out_shape=(
            jax.ShapeDtypeStruct((groups, cap, dim), BF),
            jax.ShapeDtypeStruct((groups, cap, dim), BF),
            jax.ShapeDtypeStruct((groups, cap, LANES), F32),
            jax.ShapeDtypeStruct(w.shape, BF),
        ),
        grid_spec=pltpu.PrefetchScalarGridSpec(
            num_scalar_prefetch=1,
            grid=(groups, steps),
            in_specs=[
                pl.BlockSpec((1, TILE, dim), row_map),
                pl.BlockSpec((1, TILE, dim), row_map),
                pl.BlockSpec((1, TILE, LANES), row_map),
                pl.BlockSpec((1, slices, 3, depth, ff), lambda z, i, t: (z, 0, 0, 0, 0)),
            ],
            out_specs=[
                pl.BlockSpec((1, TILE, dim), out_map),
                pl.BlockSpec((1, TILE, dim), out_map),
                pl.BlockSpec((1, TILE, LANES), out_map),
                pl.BlockSpec((1, slices, 3, depth, ff), lambda z, i, t: (z, 0, 0, 0, 0)),
            ],
            scratch_shapes=[pltpu.VMEM((dim, ff), F32)] * 3,
        ),
        compiler_params=pltpu.CompilerParams(
            dimension_semantics=("arbitrary", "arbitrary"), vmem_limit_bytes=56 << 20
        ),
        cost_estimate=pl.CostEstimate(
            flops=18 * groups * 4 * TILE * dim * ff, bytes_accessed=groups * 4 * TILE * dim * 8, transcendentals=0
        ),
        name=f"experts_{j}",
    )(tiles, hs, dys, wr, w)


def combine_kernel(first, experts, n_local, cnt, start, rank_ref, w_ref, *refs):
    outs, dhs, dws = refs[:n_local], refs[n_local:2 * n_local], refs[2 * n_local:3 * n_local]
    y_ref, dn_ref, dk_ref, obuf, dbuf, kbuf, sel, spread, ox, dx, kx, sem, xsem = refs[3 * n_local:]
    i = pl.program_id(0)
    n = pl.num_programs(0)
    slot = lax.rem(i, 2)
    lane = lax.broadcasted_iota(jnp.int32, (CHUNK, LANES), 1)
    row_lane = lax.broadcasted_iota(jnp.int32, (SEG, LANES), 1)

    def copies(step, s, e):
        z, j = divmod(e, n_local)
        at = pl.multiple_of(start[(step + first) * experts + e], 16)
        return (
            pltpu.make_async_copy(outs[j].at[z, pl.ds(at, SEG)], obuf.at[s, pl.ds(e * SEG, SEG)], sem.at[s, 0, e]),
            pltpu.make_async_copy(dhs[j].at[z, pl.ds(at, SEG)], dbuf.at[s, pl.ds(e * SEG, SEG)], sem.at[s, 1, e]),
            pltpu.make_async_copy(dws[j].at[z, pl.ds(at, SEG)], kbuf.at[s, pl.ds(e * SEG, SEG)], sem.at[s, 2, e]),
        )

    @pl.when(i == 0)
    def _():
        for e in range(experts):
            for cp in copies(0, 0, e):
                cp.start()

    @pl.when(i + 1 < n)
    def _():
        for e in range(experts):
            for cp in copies(i + 1, 1 - slot, e):
                cp.start()

    def split(v):
        hi = v.astype(BF).astype(F32)
        mid = (v - hi).astype(BF).astype(F32)
        low = v - hi - mid
        return hi, mid, low

    rank = rank_ref[...]
    w_parts = split(w_ref[...])
    for e in range(experts):
        same = lane == rank[:, e:e + 1]
        at = slice(e * SEG, (e + 1) * SEG)
        sel[0, :, at] = jnp.where(same, 1.0, 0.0).astype(BF)
        for p in range(3):
            sel[1 + p, :, at] = jnp.where(same, w_parts[p][:, e:e + 1], 0.0).astype(BF)

    for e in range(experts):
        for cp in copies(i, slot, e):
            cp.wait()

    def spread_of(e, value):
        parts = split(value)
        out = jnp.where(row_lane == e, parts[0], 0.0)
        out = jnp.where(row_lane == experts + e, parts[1], out)
        return jnp.where(row_lane == 2 * experts + e, parts[2], out).astype(BF)

    for e in range(experts):
        at = pl.ds(e * SEG, SEG)
        spread[at, :] = spread_of(e, kbuf[slot, at, :])
    y_ref[...] = dot(sel[1], obuf[slot]) + dot(sel[2], obuf[slot]) + dot(sel[3], obuf[slot])
    dn_ref[...] = dot(sel[0], dbuf[slot])
    dk_ref[...] = dot(sel[0], spread[...])

    for e in range(experts):
        z, j = divmod(e, n_local)

        @pl.when(cnt[(i + first) * experts + e] > SEG)
        def _():
            at = pl.multiple_of(start[(i + first) * experts + e] + SEG, 16)
            extra = (
                pltpu.make_async_copy(outs[j].at[z, pl.ds(at, SEG)], ox, xsem.at[0]),
                pltpu.make_async_copy(dhs[j].at[z, pl.ds(at, SEG)], dx, xsem.at[1]),
                pltpu.make_async_copy(dws[j].at[z, pl.ds(at, SEG)], kx, xsem.at[2]),
            )
            for cp in extra:
                cp.start()
            for cp in extra:
                cp.wait()
            same = lane + SEG == rank_ref[:, e:e + 1]
            pick = jnp.where(same, 1.0, 0.0).astype(BF)
            parts = split(w_ref[:, e:e + 1])
            for p in range(3):
                y_ref[...] += dot(jnp.where(same, parts[p], 0.0).astype(BF), ox[...])
            dn_ref[...] += dot(pick, dx[...])
            dk_ref[...] += dot(pick, spread_of(e, kx[...]))


def combine(first, tables, rank, w, outs, dhs, dws):
    tok = rank.shape[0]
    n_local = len(outs)
    groups, cap, dim = outs[0].shape
    experts = groups * n_local
    n = tok // CHUNK
    return pl.pallas_call(
        functools.partial(combine_kernel, first, experts, n_local),
        out_shape=(
            jax.ShapeDtypeStruct((tok, dim), F32),
            jax.ShapeDtypeStruct((tok, dim), F32),
            jax.ShapeDtypeStruct((tok, LANES), F32),
        ),
        grid_spec=pltpu.PrefetchScalarGridSpec(
            num_scalar_prefetch=2,
            grid=(n,),
            in_specs=[
                pl.BlockSpec((CHUNK, LANES), lambda i, *_: (i, 0)),
                pl.BlockSpec((CHUNK, LANES), lambda i, *_: (i, 0)),
            ] + [ANY] * (3 * n_local),
            out_specs=[
                pl.BlockSpec((CHUNK, dim), lambda i, *_: (i, 0)),
                pl.BlockSpec((CHUNK, dim), lambda i, *_: (i, 0)),
                pl.BlockSpec((CHUNK, LANES), lambda i, *_: (i, 0)),
            ],
            scratch_shapes=[
                pltpu.VMEM((2, experts * SEG, dim), BF),
                pltpu.VMEM((2, experts * SEG, dim), BF),
                pltpu.VMEM((2, experts * SEG, LANES), F32),
                pltpu.VMEM((4, CHUNK, experts * SEG), BF),
                pltpu.VMEM((experts * SEG, LANES), BF),
                pltpu.VMEM((SEG, dim), BF),
                pltpu.VMEM((SEG, dim), BF),
                pltpu.VMEM((SEG, LANES), F32),
                pltpu.SemaphoreType.DMA((2, 3, experts)),
                pltpu.SemaphoreType.DMA((3,)),
            ],
        ),
        compiler_params=pltpu.CompilerParams(
            dimension_semantics=("arbitrary",), vmem_limit_bytes=56 << 20
        ),
        cost_estimate=pl.CostEstimate(
            flops=8 * n * CHUNK * experts * SEG * dim, bytes_accessed=n * experts * SEG * dim * 4, transcendentals=0
        ),
        name=f"combine_{first}",
    )(*tables, rank, w, *outs, *dhs, *dws)


def layout_tables(mask):
    tok, experts = mask.shape
    n = tok // CHUNK
    m3 = mask.reshape(n, CHUNK, experts)
    before = jnp.tril(jnp.ones((CHUNK, CHUNK), BF), -1)
    rank = jnp.einsum('ts,cse->cte', before, m3.astype(BF), preferred_element_type=F32)
    rank = jnp.where(m3 > 0, rank, -1.0).astype(jnp.int32).reshape(tok, experts)
    cnt = jnp.sum(m3, axis=1).astype(jnp.int32)
    return rank, cnt


def pad_lanes(v):
    return jnp.pad(v, ((0, 0), (0, LANES - v.shape[1])))


def solution(mesh):
    ep_size = mesh.shape['ep']
    dp_size = mesh.shape['dp']
    n_dev = ep_size * dp_size
    nz, ny = ep_size // 2, 2
    fine = Mesh(mesh.devices.reshape(nz, ny, dp_size), ('z', 'y', 'b'))
    row_spec = P(('z', 'y', 'b'), None)
    exp_spec = P(('z', 'y'), None, None)
    every = ('z', 'y', 'b')
    swap = [(0, 1), (1, 0)]

    def local_block(hidden_in, topk_idx, grad_out, norm_gain, w_router, w_gate, w_up, w_down):
        tok, dim = hidden_in.shape
        experts = w_router.shape[1]
        top_k = topk_idx.shape[1]
        n_local, _, ff = w_gate.shape
        tok_total = tok * n_dev
        mine = nz * n_local
        chunks = tok // CHUNK
        per_dev = tok * top_k // experts + tok * top_k // (2 * experts)
        cap = -(-(2 * per_dev + 2 * chunks * 15) // TILE) * TILE + TILE
        depth = dim // dp_size
        y_at = lax.axis_index('y')
        b_at = lax.axis_index('b')

        at = b_at * depth
        g_sl = lax.dynamic_slice_in_dim(w_gate, at, depth, 1)
        u_sl = lax.dynamic_slice_in_dim(w_up, at, depth, 1)
        d_sl = lax.dynamic_slice_in_dim(w_down, at, depth, 2).transpose(0, 2, 1)
        offer = jnp.stack([g_sl, u_sl, d_sl], axis=1)
        weights_all = [
            lax.all_gather(offer[j], ('z', 'b')).reshape(nz, dp_size, 3, depth, ff) for j in range(n_local)
        ]

        dy_far = lax.ppermute(grad_out, 'y', swap)
        x_f = hidden_in.astype(F32)
        inv_rms = lax.rsqrt(jnp.mean(x_f * x_f, axis=-1, keepdims=True) + EPS)
        normed = (x_f * inv_rms * norm_gain).astype(BF)
        h_far = lax.ppermute(normed, 'y', swap)
        logits = jnp.dot(normed, w_router, preferred_element_type=F32)
        probs = jax.nn.softmax(logits, axis=-1)
        eye = jnp.arange(experts, dtype=jnp.int32)
        mask = jnp.zeros((tok, experts), F32)
        for k in range(top_k):
            mask = mask + (topk_idx[:, k:k + 1] == eye[None, :]).astype(F32)
        chosen = mask * probs
        chosen_sum = jnp.sum(chosen, axis=1, keepdims=True)
        weights = chosen / chosen_sum
        stats = lax.psum(jnp.stack([jnp.sum(mask, axis=0), jnp.sum(probs, axis=0)]), every)
        load_frac = stats[0] / (top_k * tok_total)
        aux_loss = ALPHA * experts * jnp.sum(load_frac * stats[1] / tok_total)

        def halves(v):
            v4 = v.reshape(tok, nz, ny, n_local)
            a, b = v4[:, :, 0].reshape(tok, mine), v4[:, :, 1].reshape(tok, mine)
            own = jnp.where(y_at == 0, a, b)
            return own, jnp.where(y_at == 0, b, a)

        m_near, m_send = halves(mask)
        w_near, w_send = halves(weights)
        far = lax.ppermute(jnp.concatenate([m_send, w_send], axis=1), 'y', swap)
        m_far, w_far = far[:, :mine], far[:, mine:]

        rank_near, cnt_near = layout_tables(m_near)
        rank_far, cnt_far = layout_tables(m_far)
        cnt = jnp.concatenate([cnt_near, cnt_far], axis=0)
        pad = (cnt + 15) // 16 * 16
        ends = jnp.cumsum(pad, axis=0)
        start = (ends - pad).reshape(-1)
        end = ends[-1]
        used = (end + TILE - 1) // TILE
        cnt = cnt.reshape(-1)

        tables = (cnt, start, end)
        rows = dispatch(0, False, tables, normed, grad_out, rank_near.T, w_near.T, cap)
        rows = dispatch(chunks, True, tables, h_far, dy_far, rank_far.T, w_far.T, cap, rows)
        outs, dhs, dws, grads = [], [], [], []
        used = used.reshape(nz, n_local)
        for j in range(n_local):
            o, dh, dw, gw = run_experts(j, n_local, used[:, j], *rows, weights_all[j])
            outs.append(o)
            dhs.append(dh)
            dws.append(dw)
            part = lax.psum_scatter(gw.reshape(nz * dp_size, 3, depth, ff), ('z', 'b'), scatter_dimension=0)
            grads.append(lax.all_gather(part, 'b'))

        y_far, dn_far, dk_far = combine(chunks, (cnt, start), pad_lanes(rank_far), pad_lanes(w_far), outs, dhs, dws)
        y_back = lax.ppermute(y_far, 'y', swap)
        dn_back = lax.ppermute(dn_far, 'y', swap)

        def total(v):
            return v[:, :mine] + v[:, mine:2 * mine] + v[:, 2 * mine:3 * mine]

        dk_back = lax.ppermute(total(dk_far), 'y', swap)
        y_near, dn_near, dk_near = combine(0, (cnt, start), pad_lanes(rank_near), pad_lanes(w_near), outs, dhs, dws)
        block_out = (x_f + (y_near + y_back)).astype(BF)

        near4 = total(dk_near).reshape(tok, nz, n_local)
        back4 = dk_back.reshape(tok, nz, n_local)
        d_weight = jnp.stack([jnp.where(y_at == 0, near4, back4), jnp.where(y_at == 0, back4, near4)], axis=2).reshape(tok, experts)
        d_chosen = (d_weight - jnp.sum(weights * d_weight, axis=1, keepdims=True)) / chosen_sum
        aux_coef = AUX_SCALE * math.sqrt(dim * experts) * experts
        d_prob = mask * d_chosen + aux_coef * load_frac[None, :]
        d_logit = probs * (d_prob - jnp.sum(probs * d_prob, axis=1, keepdims=True))
        d_logit_bf = d_logit.astype(BF)
        router_part = jnp.einsum('td,te->de', normed, d_logit_bf, preferred_element_type=F32)
        d_normed = dn_near + dn_back + jnp.einsum('te,de->td', d_logit_bf, w_router, preferred_element_type=F32)
        gain_part = jnp.sum(d_normed * x_f * inv_rms, axis=0)
        d_scaled = d_normed * norm_gain
        inv_cube = inv_rms * inv_rms * inv_rms
        grad_in = (grad_out.astype(F32) + inv_rms * d_scaled - x_f * inv_cube * jnp.mean(d_scaled * x_f, axis=-1, keepdims=True)).astype(BF)
        grad_router = lax.psum(router_part, every)
        grad_norm_gain = lax.psum(gain_part, every)

        full = jnp.stack(grads).transpose(2, 0, 1, 3, 4).reshape(3, n_local, dim, ff)
        return block_out, grad_in, aux_loss, grad_norm_gain, grad_router, full[0], full[1], full[2].transpose(0, 2, 1)

    return jax.shard_map(
        local_block,
        mesh=fine,
        in_specs=(row_spec, row_spec, row_spec, P(None), P(None, None), exp_spec, exp_spec, exp_spec),
        out_specs=(row_spec, row_spec, P(), P(None), P(None, None), exp_spec, exp_spec, exp_spec),
        check_vma=False,
    )
```

```python
import functools
import math
import jax
import jax.numpy as jnp
from jax import lax
from jax.experimental import pallas as pl
from jax.experimental.pallas import tpu as pltpu
from jax.sharding import Mesh, PartitionSpec as P

EPS = 1e-6
ALPHA = 0.001
AUX_SCALE = 0.25
BF = jnp.bfloat16
F32 = jnp.float32
CHUNK = 256
SEG = 128
TILE = 256
LANES = 128
ANY = pl.BlockSpec(memory_space=pl.ANY)


def dot(a, b, dims=((1,), (0,))):
    return lax.dot_general(a, b, (dims, ((), ())), preferred_element_type=F32)


def dispatch_kernel(first, last, experts, cnt, start, end, h_ref, dy_ref, rank_ref, w_ref, *refs):
    n_alias = 0 if first == 0 else 3
    hs, dys, wr, hbuf, dbuf, wbuf, hz, wz, hx, dx, wx, sem, xsem = refs[n_alias:]
    i = pl.program_id(0)
    c = i
    rows = lax.broadcasted_iota(jnp.int32, (SEG, CHUNK), 0)

    def copies(e, at):
        at = pl.multiple_of(at, 16)
        return (
            pltpu.make_async_copy(hbuf.at[e], hs.at[e, pl.ds(at, SEG)], sem.at[0, e]),
            pltpu.make_async_copy(dbuf.at[e], dys.at[e, pl.ds(at, SEG)], sem.at[1, e]),
            pltpu.make_async_copy(wbuf.at[e], wr.at[e, pl.ds(at, SEG)], sem.at[2, e]),
        )

    def select(e, base):
        same = rows + base == rank_ref[pl.ds(e, 1), :]
        pick = jnp.where(same, 1.0, 0.0).astype(BF)
        weight = jnp.sum(jnp.where(same, w_ref[pl.ds(e, 1), :], 0.0), axis=1, keepdims=True)
        return (
            dot(pick, h_ref[...]).astype(BF),
            dot(pick, dy_ref[...]).astype(BF),
            jnp.broadcast_to(weight, (SEG, LANES)),
        )

    def group(q, carry):
        for u in range(4):
            e = q * 4 + u
            h_rows, dy_rows, w_rows = select(e, 0)

            @pl.when(i > 0)
            def _():
                for cp in copies(e, 0):
                    cp.wait()

            hbuf[e] = h_rows
            dbuf[e] = dy_rows
            wbuf[e] = w_rows
            for cp in copies(e, start[c * experts + e]):
                cp.start()
        return carry

    lax.fori_loop(0, experts // 4, group, 0)

    def overflow(e, carry):
        @pl.when(cnt[c * experts + e] > SEG)
        def _():
            h_rows, dy_rows, w_rows = select(e, SEG)
            hx[...] = h_rows
            dx[...] = dy_rows
            wx[...] = w_rows
            at = pl.multiple_of(start[c * experts + e] + SEG, 16)
            extra = (
                pltpu.make_async_copy(hx, hs.at[e, pl.ds(at, SEG)], xsem.at[0]),
                pltpu.make_async_copy(dx, dys.at[e, pl.ds(at, SEG)], xsem.at[1]),
                pltpu.make_async_copy(wx, wr.at[e, pl.ds(at, SEG)], xsem.at[2]),
            )
            for cp in extra:
                cp.start()
            for cp in extra:
                cp.wait()

        return carry

    lax.fori_loop(0, experts, overflow, 0)

    @pl.when(i == pl.num_programs(0) - 1)
    def _():
        def drain(e, carry):
            for cp in copies(e, 0):
                cp.wait()
            return carry

        lax.fori_loop(0, experts, drain, 0)
        if last:
            hz[...] = jnp.zeros_like(hz)
            wz[...] = jnp.zeros_like(wz)

            def tail(e, carry):
                at = pl.multiple_of(end[e], 16)
                zero = (
                    pltpu.make_async_copy(hz, hs.at[e, pl.ds(at, TILE)], xsem.at[0]),
                    pltpu.make_async_copy(hz, dys.at[e, pl.ds(at, TILE)], xsem.at[1]),
                    pltpu.make_async_copy(wz, wr.at[e, pl.ds(at, TILE)], xsem.at[2]),
                )
                for cp in zero:
                    cp.start()
                for cp in zero:
                    cp.wait()
                return carry

            lax.fori_loop(0, experts, tail, 0)


def dispatch(first, last, tables, h, dy, rank_t, w_t, cap, prev=None):
    tok, dim = h.shape
    experts = rank_t.shape[0]
    n = tok // CHUNK
    shapes = (
        jax.ShapeDtypeStruct((experts, cap, dim), BF),
        jax.ShapeDtypeStruct((experts, cap, dim), BF),
        jax.ShapeDtypeStruct((experts, cap, LANES), F32),
    )
    prev = () if prev is None else prev
    return pl.pallas_call(
        functools.partial(dispatch_kernel, first, last, experts),
        out_shape=shapes,
        grid_spec=pltpu.PrefetchScalarGridSpec(
            num_scalar_prefetch=3,
            grid=(n,),
            in_specs=[
                pl.BlockSpec((CHUNK, dim), lambda i, *_: (i, 0)),
                pl.BlockSpec((CHUNK, dim), lambda i, *_: (i, 0)),
                pl.BlockSpec((experts, CHUNK), lambda i, *_: (0, i)),
                pl.BlockSpec((experts, CHUNK), lambda i, *_: (0, i)),
            ] + [ANY] * len(prev),
            out_specs=[ANY] * 3,
            scratch_shapes=[
                pltpu.VMEM((experts, SEG, dim), BF),
                pltpu.VMEM((experts, SEG, dim), BF),
                pltpu.VMEM((experts, SEG, LANES), F32),
                pltpu.VMEM((TILE, dim), BF),
                pltpu.VMEM((TILE, LANES), F32),
                pltpu.VMEM((SEG, dim), BF),
                pltpu.VMEM((SEG, dim), BF),
                pltpu.VMEM((SEG, LANES), F32),
                pltpu.SemaphoreType.DMA((3, experts)),
                pltpu.SemaphoreType.DMA((3,)),
            ],
        ),
        input_output_aliases={7 + k: k for k in range(len(prev))},
        compiler_params=pltpu.CompilerParams(
            dimension_semantics=("arbitrary",), vmem_limit_bytes=40 << 20
        ),
        cost_estimate=pl.CostEstimate(
            flops=4 * n * experts * SEG * CHUNK * dim, bytes_accessed=n * experts * SEG * dim * 4, transcendentals=0
        ),
    )(*tables, h, dy, rank_t, w_t, *prev)


def expert_kernel(tiles, offs, h_ref, dy_ref, wr_ref, *refs):
    pieces, (o_ref, dh_ref, dw_ref, gw_ref, acc) = refs[:4], refs[4:]
    z, i = pl.program_id(0), pl.program_id(1)
    used = tiles[z]
    block = pieces[0].shape[-1]
    halves = range(2)
    parts = range(len(pieces))

    def span(r):
        return pl.ds(pl.multiple_of(offs[r] * block, block), block)

    @pl.when(i == 0)
    def _():
        acc[...] = jnp.zeros_like(acc)

    @pl.when(i < used)
    def _():
        h = [h_ref[0, :, span(r)] for r in parts]
        gate = [sum(dot(h[r], pieces[r][0, f]) for r in parts) for f in halves]
        up = [sum(dot(h[r], pieces[r][0, 2 + f]) for r in parts) for f in halves]
        sig = [jax.nn.sigmoid(v) for v in gate]
        act = [gate[f] * sig[f] for f in halves]
        hidden = [(act[f] * up[f]).astype(BF) for f in halves]
        weight = wr_ref[0][:, :1]
        d_weight = jnp.zeros((h_ref.shape[1], 1), F32)
        d_out = []
        for r in parts:
            out = sum(dot(hidden[f], pieces[r][0, 4 + f]) for f in halves).astype(BF)
            o_ref[0, :, span(r)] = out
            dy_f = dy_ref[0, :, span(r)].astype(F32)
            d_weight = d_weight + jnp.sum(dy_f * out.astype(F32), axis=1, keepdims=True)
            d_out.append((dy_f * weight).astype(BF))
        dw_ref[0] = jnp.broadcast_to(d_weight, dw_ref.shape[1:])
        d_hidden = [sum(dot(d_out[r], pieces[r][0, 4 + f], ((1,), (1,))) for r in parts) for f in halves]
        d_gate = [(d_hidden[f] * up[f] * sig[f] * (1.0 + gate[f] * (1.0 - sig[f]))).astype(BF) for f in halves]
        d_up = [(d_hidden[f] * act[f]).astype(BF) for f in halves]
        for r in parts:
            dh_ref[0, :, span(r)] = sum(
                dot(d_gate[f], pieces[r][0, f], ((1,), (1,))) + dot(d_up[f], pieces[r][0, 2 + f], ((1,), (1,)))
                for f in halves
            ).astype(BF)
        hidden_t = [v.T for v in hidden]
        for r in parts:
            h_t = h[r].T
            for f in halves:
                acc[r, f] += dot(h_t, d_gate[f])
                acc[r, 2 + f] += dot(h_t, d_up[f])
                acc[r, 4 + f] += dot(hidden_t[f], d_out[r])

    @pl.when(i == used)
    def _():
        o_ref[...] = jnp.zeros_like(o_ref)
        dh_ref[...] = jnp.zeros_like(dh_ref)
        dw_ref[...] = jnp.zeros_like(dw_ref)

    @pl.when(i == pl.num_programs(1) - 1)
    def _():
        for r in parts:
            gw_ref[0, offs[r]] = acc[r].astype(BF)


def run_experts(j, n_local, tiles, offs, hs, dys, wr, pieces):
    _, cap, dim = hs.shape
    groups, kinds, depth, _ = pieces[0].shape
    slices = len(pieces)
    steps = cap // TILE
    ff = kinds // 3 * depth

    def row_map(z, i, t, _):
        return (z * n_local + j, jnp.minimum(i, jnp.maximum(t[z] - 1, 0)), 0)

    def out_map(z, i, t, _):
        return (z, jnp.minimum(i, t[z]), 0)

    return pl.pallas_call(
        expert_kernel,
        out_shape=(
            jax.ShapeDtypeStruct((groups, cap, dim), BF),
            jax.ShapeDtypeStruct((groups, cap, dim), BF),
            jax.ShapeDtypeStruct((groups, cap, LANES), F32),
            jax.ShapeDtypeStruct((groups, slices, kinds, depth, depth), BF),
        ),
        grid_spec=pltpu.PrefetchScalarGridSpec(
            num_scalar_prefetch=2,
            grid=(groups, steps),
            in_specs=[
                pl.BlockSpec((1, TILE, dim), row_map),
                pl.BlockSpec((1, TILE, dim), row_map),
                pl.BlockSpec((1, TILE, LANES), row_map),
            ] + [pl.BlockSpec((1, kinds, depth, depth), lambda z, i, *_: (z, 0, 0, 0))] * slices,
            out_specs=[
                pl.BlockSpec((1, TILE, dim), out_map),
                pl.BlockSpec((1, TILE, dim), out_map),
                pl.BlockSpec((1, TILE, LANES), out_map),
                pl.BlockSpec((1, slices, kinds, depth, depth), lambda z, i, *_: (z, 0, 0, 0, 0)),
            ],
            scratch_shapes=[pltpu.VMEM((slices, kinds, depth, depth), F32)],
        ),
        compiler_params=pltpu.CompilerParams(
            dimension_semantics=("arbitrary", "arbitrary"), vmem_limit_bytes=56 << 20
        ),
        cost_estimate=pl.CostEstimate(
            flops=18 * groups * 4 * TILE * dim * ff, bytes_accessed=groups * 4 * TILE * dim * 8, transcendentals=0
        ),
    )(tiles, offs, hs, dys, wr, *pieces)


def combine_kernel(experts, n_local, cnt, start, rank_ref, w_ref, *refs):
    outs, dhs, dws = refs[:n_local], refs[n_local:2 * n_local], refs[2 * n_local:3 * n_local]
    y_ref, dn_ref, dk_ref, obuf, dbuf, kbuf, sel, spread, ox, dx, kx, sem, xsem = refs[3 * n_local:]
    i = pl.program_id(0)
    n = pl.num_programs(0)
    slot = lax.rem(i, 2)
    lane = lax.broadcasted_iota(jnp.int32, (CHUNK, LANES), 1)
    row_lane = lax.broadcasted_iota(jnp.int32, (SEG, LANES), 1)

    def copies(step, s, e):
        z, j = divmod(e, n_local)
        at = pl.multiple_of(start[step * experts + e], 16)
        return (
            pltpu.make_async_copy(outs[j].at[z, pl.ds(at, SEG)], obuf.at[s, pl.ds(e * SEG, SEG)], sem.at[s, 0, e]),
            pltpu.make_async_copy(dhs[j].at[z, pl.ds(at, SEG)], dbuf.at[s, pl.ds(e * SEG, SEG)], sem.at[s, 1, e]),
            pltpu.make_async_copy(dws[j].at[z, pl.ds(at, SEG)], kbuf.at[s, pl.ds(e * SEG, SEG)], sem.at[s, 2, e]),
        )

    @pl.when(i == 0)
    def _():
        for e in range(experts):
            for cp in copies(0, 0, e):
                cp.start()

    @pl.when(i + 1 < n)
    def _():
        for e in range(experts):
            for cp in copies(i + 1, 1 - slot, e):
                cp.start()

    def split(v):
        hi = v.astype(BF).astype(F32)
        mid = (v - hi).astype(BF).astype(F32)
        low = v - hi - mid
        return hi, mid, low

    rank = rank_ref[...]
    w_parts = split(w_ref[...])
    for e in range(experts):
        same = lane == rank[:, e:e + 1]
        at = slice(e * SEG, (e + 1) * SEG)
        sel[0, :, at] = jnp.where(same, 1.0, 0.0).astype(BF)
        for p in range(3):
            sel[1 + p, :, at] = jnp.where(same, w_parts[p][:, e:e + 1], 0.0).astype(BF)

    for e in range(experts):
        for cp in copies(i, slot, e):
            cp.wait()

    def spread_of(e, value):
        parts = split(value)
        out = jnp.where(row_lane == e, parts[0], 0.0)
        out = jnp.where(row_lane == experts + e, parts[1], out)
        return jnp.where(row_lane == 2 * experts + e, parts[2], out).astype(BF)

    for e in range(experts):
        at = pl.ds(e * SEG, SEG)
        spread[at, :] = spread_of(e, kbuf[slot, at, :])
    y_ref[...] = dot(sel[1], obuf[slot]) + dot(sel[2], obuf[slot]) + dot(sel[3], obuf[slot])
    dn_ref[...] = dot(sel[0], dbuf[slot])
    dk_ref[...] = dot(sel[0], spread[...])

    for e in range(experts):
        z, j = divmod(e, n_local)

        @pl.when(cnt[i * experts + e] > SEG)
        def _():
            at = pl.multiple_of(start[i * experts + e] + SEG, 16)
            extra = (
                pltpu.make_async_copy(outs[j].at[z, pl.ds(at, SEG)], ox, xsem.at[0]),
                pltpu.make_async_copy(dhs[j].at[z, pl.ds(at, SEG)], dx, xsem.at[1]),
                pltpu.make_async_copy(dws[j].at[z, pl.ds(at, SEG)], kx, xsem.at[2]),
            )
            for cp in extra:
                cp.start()
            for cp in extra:
                cp.wait()
            same = lane + SEG == rank_ref[:, e:e + 1]
            pick = jnp.where(same, 1.0, 0.0).astype(BF)
            parts = split(w_ref[:, e:e + 1])
            for p in range(3):
                y_ref[...] += dot(jnp.where(same, parts[p], 0.0).astype(BF), ox[...])
            dn_ref[...] += dot(pick, dx[...])
            dk_ref[...] += dot(pick, spread_of(e, kx[...]))


def combine(tables, rank, w, outs, dhs, dws):
    tok = rank.shape[0]
    n_local = len(outs)
    groups, _, dim = outs[0].shape
    experts = groups * n_local
    n = tok // CHUNK
    return pl.pallas_call(
        functools.partial(combine_kernel, experts, n_local),
        out_shape=(
            jax.ShapeDtypeStruct((tok, dim), F32),
            jax.ShapeDtypeStruct((tok, dim), F32),
            jax.ShapeDtypeStruct((tok, LANES), F32),
        ),
        grid_spec=pltpu.PrefetchScalarGridSpec(
            num_scalar_prefetch=2,
            grid=(n,),
            in_specs=[
                pl.BlockSpec((CHUNK, LANES), lambda i, *_: (i, 0)),
                pl.BlockSpec((CHUNK, LANES), lambda i, *_: (i, 0)),
            ] + [ANY] * (3 * n_local),
            out_specs=[
                pl.BlockSpec((CHUNK, dim), lambda i, *_: (i, 0)),
                pl.BlockSpec((CHUNK, dim), lambda i, *_: (i, 0)),
                pl.BlockSpec((CHUNK, LANES), lambda i, *_: (i, 0)),
            ],
            scratch_shapes=[
                pltpu.VMEM((2, experts * SEG, dim), BF),
                pltpu.VMEM((2, experts * SEG, dim), BF),
                pltpu.VMEM((2, experts * SEG, LANES), F32),
                pltpu.VMEM((4, CHUNK, experts * SEG), BF),
                pltpu.VMEM((experts * SEG, LANES), BF),
                pltpu.VMEM((SEG, dim), BF),
                pltpu.VMEM((SEG, dim), BF),
                pltpu.VMEM((SEG, LANES), F32),
                pltpu.SemaphoreType.DMA((2, 3, experts)),
                pltpu.SemaphoreType.DMA((3,)),
            ],
        ),
        compiler_params=pltpu.CompilerParams(
            dimension_semantics=("arbitrary",), vmem_limit_bytes=56 << 20
        ),
        cost_estimate=pl.CostEstimate(
            flops=8 * n * CHUNK * experts * SEG * dim, bytes_accessed=n * experts * SEG * dim * 4, transcendentals=0
        ),
        name="combine",
    )(*tables, rank, w, *outs, *dhs, *dws)


def small_sum_kernel(axes, sizes, whole_ref, split_ref, whole_out, split_out, got_w, got_s, mine, send, recv):
    n = math.prod(sizes)
    me = 0
    for axis, size in zip(axes, sizes):
        me = me * size + lax.axis_index(axis)

    def place(p):
        out = []
        for size in reversed(sizes):
            out.append(lax.rem(p, size))
            p = p // size
        return tuple(reversed(out))

    barrier = pltpu.get_barrier_semaphore()
    for k in range(1, n):
        pl.semaphore_signal(barrier, inc=1, device_id=place(lax.rem(me + k, n)), device_id_type=pl.DeviceIdType.MESH)
    pl.semaphore_wait(barrier, n - 1)

    def copy(src, dst, what, k):
        peer = lax.rem(me + k, n)
        return pltpu.make_async_remote_copy(
            src_ref=src, dst_ref=dst, send_sem=send.at[what, k], recv_sem=recv.at[what, k],
            device_id=place(peer), device_id_type=pl.DeviceIdType.MESH,
        )

    def rows_of(p):
        return split_ref.at[pl.ds(pl.multiple_of(p * 8, 8), 8)]

    first = []
    for k in range(1, n):
        first.append(copy(whole_ref, got_w.at[me], 0, k))
        if split_ref is not None:
            first.append(copy(rows_of(lax.rem(me + k, n)), got_s.at[me], 1, k))
    for cp in first:
        cp.start()
    got_w[me] = whole_ref[...]
    if split_ref is not None:
        got_s[me] = split_ref[pl.ds(pl.multiple_of(me * 8, 8), 8)]
    for cp in first:
        cp.wait()
    whole_out[...] = jnp.sum(got_w[...], axis=0)
    if split_ref is not None:
        mine[...] = jnp.sum(got_s[...], axis=0)
        own = pl.ds(pl.multiple_of(me * 8, 8), 8)
        split_out[own, :] = mine[...]
        second = [copy(mine, split_out.at[own], 2, k) for k in range(1, n)]
        for cp in second:
            cp.start()
        for cp in second:
            cp.wait()


def small_sum(axes, sizes, ident, whole, split=None):
    n = math.prod(sizes)
    vmem = pl.BlockSpec(memory_space=pltpu.VMEM)
    scratch = [pltpu.VMEM((n,) + whole.shape, F32)]
    if split is not None:
        scratch += [pltpu.VMEM((n, 8, LANES), F32), pltpu.VMEM((8, LANES), F32)]
    scratch += [pltpu.SemaphoreType.DMA((3, n)), pltpu.SemaphoreType.DMA((3, n))]
    kernel = functools.partial(small_sum_kernel, axes, sizes)
    if split is None:
        def body(w, wo, gw, ss, rs):
            kernel(w, None, wo, None, gw, None, None, ss, rs)

        args = (whole,)
    else:
        body = kernel
        args = (whole, split)
    out = pl.pallas_call(
        body,
        out_shape=tuple(jax.ShapeDtypeStruct(v.shape, F32) for v in args),
        in_specs=[vmem] * len(args),
        out_specs=tuple([vmem] * len(args)),
        scratch_shapes=scratch,
        compiler_params=pltpu.CompilerParams(collective_id=ident, has_side_effects=True),
    )(*args)
    return out


def assemble_kernel(slices, sizes, offs, *refs):
    groups = len(sizes)
    pieces = [refs[g * slices:(g + 1) * slices] for g in range(groups)]
    gate, up, down, buf, sem_in, sem_out = refs[groups * slices:]
    block = buf.shape[-1]
    base = [sum(sizes[:g]) for g in range(groups)]
    loads = [
        [pltpu.make_async_copy(pieces[g][r], buf.at[r, pl.ds(base[g], sizes[g])], sem_in.at[g, r]) for r in range(slices)]
        for g in range(groups)
    ]
    for g in range(groups):
        for r in range(slices):
            loads[g][r].start()
    stores = []
    for g in range(groups):
        experts = pl.ds(base[g], sizes[g])
        for r in range(slices):
            loads[g][r].wait()
            at = pl.ds(pl.multiple_of(offs[r] * block, block), block)
            for f in range(2):
                part = pl.ds(f * block, block)
                for t, target in enumerate((gate.at[experts, at, part], up.at[experts, at, part], down.at[experts, part, at])):
                    cp = pltpu.make_async_copy(buf.at[r, experts, 2 * t + f], target, sem_out.at[g, r, 2 * t + f])
                    cp.start()
                    stores.append(cp)
    for cp in stores:
        cp.wait()


def assemble(offs, groups, shapes):
    slices = len(groups[0])
    sizes = [g[0].shape[0] for g in groups]
    kinds, depth = groups[0][0].shape[1:3]
    flat = [p for g in groups for p in g]
    return pl.pallas_call(
        functools.partial(assemble_kernel, slices, sizes),
        out_shape=tuple(jax.ShapeDtypeStruct(v, BF) for v in shapes),
        grid_spec=pltpu.PrefetchScalarGridSpec(
            num_scalar_prefetch=1,
            grid=(),
            in_specs=[ANY] * len(flat),
            out_specs=[ANY] * 3,
            scratch_shapes=[
                pltpu.VMEM((slices, sum(sizes), kinds, depth, depth), BF),
                pltpu.SemaphoreType.DMA((len(sizes), slices)),
                pltpu.SemaphoreType.DMA((len(sizes), slices, kinds)),
            ],
        ),
        compiler_params=pltpu.CompilerParams(vmem_limit_bytes=24 << 20),
        name="assemble",
    )(offs, *flat)


def layout_tables(mask):
    tok, experts = mask.shape
    n = tok // CHUNK
    m3 = mask.reshape(n, CHUNK, experts)
    before = jnp.tril(jnp.ones((CHUNK, CHUNK), BF), -1)
    rank = jnp.einsum('ts,cse->cte', before, m3.astype(BF), preferred_element_type=F32)
    rank = jnp.where(m3 > 0, rank, -1.0).astype(jnp.int32).reshape(tok, experts)
    cnt = jnp.sum(m3, axis=1).astype(jnp.int32)
    return rank, cnt


def pad_lanes(v):
    return jnp.pad(v, ((0, 0), (0, LANES - v.shape[1])))


def solution(mesh):
    ep_size = mesh.shape['ep']
    dp_size = mesh.shape['dp']
    n_dev = ep_size * dp_size
    nz, ny = ep_size // 2, 2
    fine = Mesh(mesh.devices.reshape(nz, ny, dp_size), ('z', 'y', 'b'))
    row_spec = P(('z', 'y', 'b'), None)
    exp_spec = P(('z', 'y'), None, None)
    every = ('z', 'y', 'b')
    counts_of = (nz, ny, dp_size)
    swap = [(0, 1), (1, 0)]
    to_x = [(q, q ^ 2) for q in range(dp_size)]
    to_core = [(q, q ^ 1) for q in range(dp_size)]

    def spread_slices(own):
        other_x = lax.ppermute(own, 'b', to_x)
        return (own, lax.ppermute(own, 'b', to_core), other_x, lax.ppermute(other_x, 'b', to_core))

    def block_of(hidden_in, topk_idx, grad_out, norm_gain, w_router, w_gate, w_up, w_down):
        tok, dim = hidden_in.shape
        experts = w_router.shape[1]
        top_k = topk_idx.shape[1]
        n_local, _, ff = w_gate.shape
        tok_total = tok * n_dev
        mine = nz * n_local
        chunks = tok // CHUNK
        per_dev = tok * top_k // experts + tok * top_k // (2 * experts)
        cap = -(-(2 * per_dev + 2 * chunks * 15) // TILE) * TILE + TILE
        depth = dim // dp_size
        y_at = lax.axis_index('y')
        b_at = lax.axis_index('b')
        offs = jnp.bitwise_xor(b_at, jnp.arange(dp_size, dtype=jnp.int32))

        dy_far = lax.ppermute(grad_out, 'y', swap)
        at = b_at * depth

        def blocks(w):
            part = lax.dynamic_slice_in_dim(w, at, depth, 1)
            return part.reshape(n_local, depth, ff // depth, depth).transpose(0, 2, 1, 3)

        d_sl = lax.dynamic_slice_in_dim(w_down, at, depth, 2).reshape(n_local, ff // depth, depth, depth)
        offer = jnp.concatenate([blocks(w_gate), blocks(w_up), d_sl], axis=1)
        pieces = []
        for j in range(n_local):
            gathered = lax.all_gather(offer[j], 'z')
            pieces.append(spread_slices(gathered))

        x_f = hidden_in.astype(F32)
        inv_rms = lax.rsqrt(jnp.mean(x_f * x_f, axis=-1, keepdims=True) + EPS)
        normed = (x_f * inv_rms * norm_gain).astype(BF)
        h_far = lax.ppermute(normed, 'y', swap)
        logits = jnp.dot(normed, w_router, preferred_element_type=F32)
        probs = jax.nn.softmax(logits, axis=-1)
        eye = jnp.arange(experts, dtype=jnp.int32)
        mask = jnp.zeros((tok, experts), F32)
        for k in range(top_k):
            mask = mask + (topk_idx[:, k:k + 1] == eye[None, :]).astype(F32)
        chosen = mask * probs
        chosen_sum = jnp.sum(chosen, axis=1, keepdims=True)
        weights = chosen / chosen_sum

        def halves(v):
            v4 = v.reshape(tok, nz, ny, n_local)
            a, b = v4[:, :, 0].reshape(tok, mine), v4[:, :, 1].reshape(tok, mine)
            own = jnp.where(y_at == 0, a, b)
            return own, jnp.where(y_at == 0, b, a)

        m_near, m_send = halves(mask)
        w_near, w_send = halves(weights)
        far = lax.ppermute(jnp.concatenate([m_send, w_send], axis=1), 'y', swap)
        m_far, w_far = far[:, :mine], far[:, mine:]

        rank_near, cnt_near = layout_tables(m_near)
        pad_near = (cnt_near + 15) // 16 * 16
        end_near = jnp.cumsum(pad_near, axis=0)
        near = (cnt_near.reshape(-1), (end_near - pad_near).reshape(-1), end_near[-1])
        rank_far, cnt_far = layout_tables(m_far)
        pad_far = (cnt_far + 15) // 16 * 16
        end_far = jnp.cumsum(pad_far, axis=0) + end_near[-1]
        end = end_far[-1]
        far_t = (cnt_far.reshape(-1), (end_far - pad_far).reshape(-1), end)
        used = ((end + TILE - 1) // TILE).reshape(nz, n_local)

        rows = dispatch(0, False, near, normed, grad_out, rank_near.T, w_near.T, cap)
        rows = dispatch(1, True, far_t, h_far, dy_far, rank_far.T, w_far.T, cap, rows)

        stats_in = jnp.pad(jnp.stack([jnp.sum(mask, axis=0), jnp.sum(probs, axis=0)]), ((0, 6), (0, LANES - experts)))
        stats_in, marks = lax.optimization_barrier((stats_in, rows[2]))
        (stats,) = small_sum(every, counts_of, 0, stats_in)
        used, stats = lax.optimization_barrier((used, stats))
        rows = (rows[0], rows[1], marks)
        load_frac = stats[0, :experts] / (top_k * tok_total)
        aux_loss = ALPHA * experts * jnp.sum(load_frac * stats[1, :experts] / tok_total)

        outs, dhs, dws, sums = [], [], [], []
        for j in range(n_local):
            o, dh, dw, gw = run_experts(j, n_local, used[:, j], offs, *rows, pieces[j])
            used, dw = lax.optimization_barrier((used, dw))
            outs.append(o)
            dhs.append(dh)
            dws.append(dw)
            sums.append(lax.psum_scatter(gw.reshape((nz * dp_size,) + gw.shape[2:]), ('z', 'b'), scatter_dimension=0))

        def total(v):
            return v[:, :mine] + v[:, mine:2 * mine] + v[:, 2 * mine:3 * mine]

        y_far, dn_far, dk_far = combine(far_t[:2], pad_lanes(rank_far), pad_lanes(w_far), outs, dhs, dws)
        dk_back = lax.ppermute(total(dk_far), 'y', swap)
        y_back = lax.ppermute(y_far, 'y', swap)
        dn_back = lax.ppermute(dn_far, 'y', swap)
        y_near, dn_near, dk_near = combine(near[:2], pad_lanes(rank_near), pad_lanes(w_near), outs, dhs, dws)

        *early, y_near = lax.optimization_barrier((*sums[:-1], y_near))
        late, y_near = lax.optimization_barrier((sums[-1], y_near))
        grads = assemble(
            offs,
            [spread_slices(jnp.stack(early)), spread_slices(late[None])],
            (w_gate.shape, w_up.shape, w_down.shape),
        )
        block_out = (x_f + (y_near + y_back)).astype(BF)

        near4 = total(dk_near).reshape(tok, nz, n_local)
        back4 = dk_back.reshape(tok, nz, n_local)
        d_weight = jnp.stack([jnp.where(y_at == 0, near4, back4), jnp.where(y_at == 0, back4, near4)], axis=2).reshape(tok, experts)
        d_chosen = (d_weight - jnp.sum(weights * d_weight, axis=1, keepdims=True)) / chosen_sum
        aux_coef = AUX_SCALE * math.sqrt(dim * experts) * experts
        d_prob = mask * d_chosen + aux_coef * load_frac[None, :]
        d_logit = probs * (d_prob - jnp.sum(probs * d_prob, axis=1, keepdims=True))
        d_logit_bf = d_logit.astype(BF)
        router_part = jnp.einsum('td,te->de', normed, d_logit_bf, preferred_element_type=F32)
        d_normed = dn_near + dn_back + jnp.einsum('te,de->td', d_logit_bf, w_router, preferred_element_type=F32)
        gain_part = jnp.sum(d_normed * x_f * inv_rms, axis=0)
        d_scaled = d_normed * norm_gain
        inv_cube = inv_rms * inv_rms * inv_rms
        grad_in = (grad_out.astype(F32) + inv_rms * d_scaled - x_f * inv_cube * jnp.mean(d_scaled * x_f, axis=-1, keepdims=True)).astype(BF)
        gain_sum, router_sum = small_sum(
            every, counts_of, 1, gain_part.reshape(-1, LANES), router_part.reshape(-1, LANES)
        )
        return (block_out, grad_in, aux_loss, gain_sum.reshape(dim), router_sum.reshape(dim, experts), *grads)


    return jax.shard_map(
        block_of,
        mesh=fine,
        in_specs=(row_spec, row_spec, row_spec, P(None), P(None, None), exp_spec, exp_spec, exp_spec),
        out_specs=(row_spec, row_spec, P(), P(None), P(None, None), exp_spec, exp_spec, exp_spec),
        check_vma=False,
    )
```

```python
import functools
import math
import jax
import jax.numpy as jnp
from jax import lax
from jax.experimental import pallas as pl
from jax.experimental.pallas import tpu as pltpu
from jax.sharding import Mesh, PartitionSpec as P


EPS = 1e-6
ALPHA = 0.001
AUX_SCALE = 0.25
BF = jnp.bfloat16
F32 = jnp.float32
CHUNK = 256
FAR_PARTS = 2
GROUP = 4
SEG = 128
ALIGN = 8
TILE = 256
LANES = 128
ANY = pl.BlockSpec(memory_space=pl.ANY)


def dot(a, b, dims=((1,), (0,))):
    return lax.dot_general(a, b, (dims, ((), ())), preferred_element_type=F32)


def offer_kernel(at_ref, gate, up, down, *refs):
    outs, (buf, sem_in, sem_out) = refs[:-3], refs[-3:]
    depth = buf.shape[-1]
    at = pl.ds(pl.multiple_of(at_ref[0] * depth, depth), depth)
    loads = []
    for j in range(len(outs)):
        mine = []
        for f in range(2):
            half = pl.ds(f * depth, depth)
            for t, src in enumerate((gate.at[j, at, half], up.at[j, at, half], down.at[j, half, at])):
                mine.append(pltpu.make_async_copy(src, buf.at[j, 2 * t + f], sem_in.at[j, 2 * t + f]))
        for cp in mine:
            cp.start()
        loads.append(mine)
    stores = []
    for j, mine in enumerate(loads):
        for cp in mine:
            cp.wait()
        stores.append(pltpu.make_async_copy(buf.at[j], outs[j], sem_out.at[j]))
        stores[-1].start()
    for cp in stores:
        cp.wait()


def offer(at, w_gate, w_up, w_down, depth):
    n_local = w_gate.shape[0]
    kinds = 3 * w_gate.shape[2] // depth
    return pl.pallas_call(
        offer_kernel,
        out_shape=tuple([jax.ShapeDtypeStruct((kinds, depth, depth), BF)] * n_local),
        grid_spec=pltpu.PrefetchScalarGridSpec(
            num_scalar_prefetch=1,
            grid=(),
            in_specs=[ANY] * 3,
            out_specs=[ANY] * n_local,
            scratch_shapes=[
                pltpu.VMEM((n_local, kinds, depth, depth), BF),
                pltpu.SemaphoreType.DMA((n_local, kinds)),
                pltpu.SemaphoreType.DMA((n_local,)),
            ],
        ),
        name="offer",
    )(at, w_gate, w_up, w_down)


def others_kernel(at_ref, src, out, buf, sem_in, sem_out):
    n = src.shape[0]
    loads = [
        pltpu.make_async_copy(src.at[lax.rem(at_ref[0] + 1 + q, n)], buf.at[q], sem_in.at[q]) for q in range(n - 1)
    ]
    stores = [pltpu.make_async_copy(buf.at[q], out.at[q], sem_out.at[q]) for q in range(n - 1)]
    for cp in loads:
        cp.start()
    for load, store in zip(loads, stores):
        load.wait()
        store.start()
    for cp in stores:
        cp.wait()


def others_of(at, gathered):
    n = gathered.shape[0]
    shape = (n - 1,) + gathered.shape[1:]
    return pl.pallas_call(
        others_kernel,
        out_shape=jax.ShapeDtypeStruct(shape, BF),
        grid_spec=pltpu.PrefetchScalarGridSpec(
            num_scalar_prefetch=1,
            grid=(),
            in_specs=[ANY],
            out_specs=ANY,
            scratch_shapes=[pltpu.VMEM(shape, BF), pltpu.SemaphoreType.DMA((n - 1,)), pltpu.SemaphoreType.DMA((n - 1,))],
        ),
        name="others",
    )(at, gathered)


def dispatch_kernel(first, last, experts, cnt, start, end, h_ref, dy_ref, rank_ref, w_ref, *refs):
    n_alias = 0 if first == 0 else 3
    hs, dys, wr, hbuf, dbuf, wbuf, hz, wz, hx, dx, wx, sem, xsem = refs[n_alias:]
    i = pl.program_id(0)
    c = i
    rows = lax.broadcasted_iota(jnp.int32, (SEG, CHUNK), 0)

    def copies(e, at):
        at = pl.multiple_of(at, ALIGN)
        return (
            pltpu.make_async_copy(hbuf.at[e], hs.at[e, pl.ds(at, SEG)], sem.at[0, e]),
            pltpu.make_async_copy(dbuf.at[e], dys.at[e, pl.ds(at, SEG)], sem.at[1, e]),
            pltpu.make_async_copy(wbuf.at[e], wr.at[e, pl.ds(at, SEG)], sem.at[2, e]),
        )

    def pick_of(e, base):
        same = rows + base == rank_ref[pl.ds(e, 1), :]
        weight = jnp.sum(jnp.where(same, w_ref[pl.ds(e, 1), :], 0.0), axis=1, keepdims=True)
        return jnp.where(same, 1.0, 0.0).astype(BF), jnp.broadcast_to(weight, (SEG, LANES))

    def group(q, carry):
        found = [pick_of(q * GROUP + u, 0) for u in range(GROUP)]
        pick = jnp.concatenate([v[0] for v in found], axis=0)
        for buf, src, what in ((hbuf, h_ref, 0), (dbuf, dy_ref, 1)):
            got = dot(pick, src[...]).astype(BF)

            @pl.when(i > 0)
            def _():
                for u in range(GROUP):
                    copies(q * GROUP + u, 0)[what].wait()

            for u in range(GROUP):
                e = q * GROUP + u
                buf[e] = got[u * SEG:(u + 1) * SEG]
                copies(e, start[c * experts + e])[what].start()

        @pl.when(i > 0)
        def _():
            for u in range(GROUP):
                copies(q * GROUP + u, 0)[2].wait()

        for u in range(GROUP):
            e = q * GROUP + u
            wbuf[e] = found[u][1]
            copies(e, start[c * experts + e])[2].start()
        return carry

    lax.fori_loop(0, experts // GROUP, group, 0)

    def overflow(e, carry):
        @pl.when(cnt[c * experts + e] > SEG)
        def _():
            pick, weight = pick_of(e, SEG)
            hx[...] = dot(pick, h_ref[...]).astype(BF)
            dx[...] = dot(pick, dy_ref[...]).astype(BF)
            wx[...] = weight
            at = pl.multiple_of(start[c * experts + e] + SEG, ALIGN)
            extra = (
                pltpu.make_async_copy(hx, hs.at[e, pl.ds(at, SEG)], xsem.at[0]),
                pltpu.make_async_copy(dx, dys.at[e, pl.ds(at, SEG)], xsem.at[1]),
                pltpu.make_async_copy(wx, wr.at[e, pl.ds(at, SEG)], xsem.at[2]),
            )
            for cp in extra:
                cp.start()
            for cp in extra:
                cp.wait()

        return carry

    lax.fori_loop(0, experts, overflow, 0)

    @pl.when(i == pl.num_programs(0) - 1)
    def _():
        def drain(e, carry):
            for cp in copies(e, 0):
                cp.wait()
            return carry

        lax.fori_loop(0, experts, drain, 0)
        if last:
            hz[...] = jnp.zeros_like(hz)
            wz[...] = jnp.zeros_like(wz)

            def fills(e):
                at = pl.multiple_of(end[e], ALIGN)
                return (
                    pltpu.make_async_copy(hz, hs.at[e, pl.ds(at, TILE)], sem.at[0, e]),
                    pltpu.make_async_copy(hz, dys.at[e, pl.ds(at, TILE)], sem.at[1, e]),
                    pltpu.make_async_copy(wz, wr.at[e, pl.ds(at, TILE)], sem.at[2, e]),
                )

            def fill(e, carry):
                for cp in fills(e):
                    cp.start()
                return carry

            def filled(e, carry):
                for cp in fills(e):
                    cp.wait()
                return carry

            lax.fori_loop(0, experts, fill, 0)
            lax.fori_loop(0, experts, filled, 0)


def dispatch(first, last, tables, h, dy, rank_t, w_t, cap, prev=None):
    tok, dim = h.shape
    experts = rank_t.shape[0]
    n = tok // CHUNK
    skip = max(first - 1, 0) * n
    shapes = (
        jax.ShapeDtypeStruct((experts, cap, dim), BF),
        jax.ShapeDtypeStruct((experts, cap, dim), BF),
        jax.ShapeDtypeStruct((experts, cap, LANES), F32),
    )
    prev = () if prev is None else prev
    return pl.pallas_call(
        functools.partial(dispatch_kernel, first, last, experts),
        out_shape=shapes,
        grid_spec=pltpu.PrefetchScalarGridSpec(
            num_scalar_prefetch=3,
            grid=(n,),
            in_specs=[
                pl.BlockSpec((CHUNK, dim), lambda i, *_: (i, 0)),
                pl.BlockSpec((CHUNK, dim), lambda i, *_: (i + skip, 0)),
                pl.BlockSpec((experts, CHUNK), lambda i, *_: (0, i)),
                pl.BlockSpec((experts, CHUNK), lambda i, *_: (0, i)),
            ] + [ANY] * len(prev),
            out_specs=[ANY] * 3,
            scratch_shapes=[
                pltpu.VMEM((experts, SEG, dim), BF),
                pltpu.VMEM((experts, SEG, dim), BF),
                pltpu.VMEM((experts, SEG, LANES), F32),
                pltpu.VMEM((TILE, dim), BF),
                pltpu.VMEM((TILE, LANES), F32),
                pltpu.VMEM((SEG, dim), BF),
                pltpu.VMEM((SEG, dim), BF),
                pltpu.VMEM((SEG, LANES), F32),
                pltpu.SemaphoreType.DMA((3, experts)),
                pltpu.SemaphoreType.DMA((3,)),
            ],
        ),
        input_output_aliases={7 + k: k for k in range(len(prev))},
        compiler_params=pltpu.CompilerParams(
            dimension_semantics=("arbitrary",), vmem_limit_bytes=40 << 20
        ),
        cost_estimate=pl.CostEstimate(
            flops=4 * n * experts * SEG * CHUNK * dim, bytes_accessed=n * experts * SEG * dim * 4, transcendentals=0
        ),
    )(*tables, h, dy, rank_t, w_t, *prev)


def expert_kernel(j, item_z, item_t, item_at, tiles, offs, total, h_ref, dy_ref, wr_ref, *refs):
    own, remote, (o_ref, dh_ref, dw_ref, gw_ref, acc_gu, acc_d, wbuf, sem) = refs[:3], refs[3:7], refs[7:]
    k = pl.program_id(0)
    i = item_t[k]
    turn = item_z[k]
    slot = lax.rem(turn, 2)
    live = k < total[0]
    block = wbuf.shape[-1]
    halves = range(2)
    parts = range(len(remote))

    def span(r):
        return pl.ds(pl.multiple_of(offs[r] * block, block), block)

    def own_copies():
        out = []
        for r in parts:
            for f in halves:
                half = pl.ds(f * block, block)
                for t, src in enumerate((own[0].at[j, span(r), half], own[1].at[j, span(r), half], own[2].at[j, half, span(r)])):
                    out.append(pltpu.make_async_copy(src, wbuf.at[0, r, 2 * t + f], sem.at[0, r, 2 * t + f]))
        return out

    def remote_copies(which):
        at = lax.rem(which, 2)
        return [pltpu.make_async_copy(remote[r].at[which - 1], wbuf.at[at, r], sem.at[at, r, 6]) for r in parts]

    @pl.when(k == 0)
    def _():
        for cp in own_copies():
            cp.start()
        for cp in own_copies():
            cp.wait()

    @pl.when(live & (i == 0) & (turn > 0))
    def _():
        for cp in remote_copies(turn):
            cp.wait()

    @pl.when(live & (i == 0) & (turn + 1 < tiles.shape[0]))
    def _():
        for cp in remote_copies(turn + 1):
            cp.start()

    @pl.when(live & (i == 0))
    def _():
        acc_gu[...] = jnp.zeros_like(acc_gu)
        acc_d[...] = jnp.zeros_like(acc_d)

    @pl.when(live)
    def _():
        h = [h_ref[0, :, span(r)] for r in parts]
        gate = [sum(dot(h[r], wbuf[slot, r, f]) for r in parts) for f in halves]
        up = [sum(dot(h[r], wbuf[slot, r, 2 + f]) for r in parts) for f in halves]
        sig = [jax.nn.sigmoid(v) for v in gate]
        act = [gate[f] * sig[f] for f in halves]
        hidden = [(act[f] * up[f]).astype(BF) for f in halves]
        for r in parts:
            o_ref[0, :, span(r)] = sum(dot(hidden[f], wbuf[slot, r, 4 + f]) for f in halves).astype(BF)
        dy_f = dy_ref[0].astype(F32)
        d_out = (dy_f * wr_ref[0][:, :1]).astype(BF)
        d_weight = jnp.sum(dy_f * o_ref[0].astype(F32), axis=1, keepdims=True)
        dw_ref[0] = jnp.broadcast_to(d_weight, dw_ref.shape[1:])
        g_ref = dh_ref
        g_ref[0] = d_out
        d_parts = [g_ref[0, :, span(r)] for r in parts]
        d_hidden = [sum(dot(d_parts[r], wbuf[slot, r, 4 + f], ((1,), (1,))) for r in parts) for f in halves]
        d_gate = [(d_hidden[f] * up[f] * sig[f] * (1.0 + gate[f] * (1.0 - sig[f]))).astype(BF) for f in halves]
        d_up = [(d_hidden[f] * act[f]).astype(BF) for f in halves]
        for f in halves:
            acc_d[f] += dot(hidden[f].T, d_out)
        h_t = h_ref[0].T
        for f in halves:
            acc_gu[f] += dot(h_t, d_gate[f])
            acc_gu[2 + f] += dot(h_t, d_up[f])
        for r in parts:
            dh_ref[0, :, span(r)] = sum(
                dot(d_gate[f], wbuf[slot, r, f], ((1,), (1,))) + dot(d_up[f], wbuf[slot, r, 2 + f], ((1,), (1,)))
                for f in halves
            ).astype(BF)

    @pl.when(live & (i == tiles[turn] - 1))
    def _():
        for r in parts:
            at = slice(r * block, (r + 1) * block)
            for f in range(4):
                gw_ref[0, r, f] = acc_gu[f, at, :].astype(BF)
            for f in halves:
                gw_ref[0, r, 4 + f] = acc_d[f, :, at].astype(BF)


def run_experts(j, n_local, steps, offs, hs, dys, wr, own, remote):
    _, cap, dim = hs.shape
    others, kinds, depth, _ = remote[0].shape
    groups = others + 1
    slices = len(remote)
    ff = kinds // 3 * depth

    def row_map(k, zs, ts, at, *_):
        return (at[k] * n_local + j, ts[k], 0)

    def out_map(k, zs, ts, at, *_):
        return (at[k], ts[k], 0)

    return pl.pallas_call(
        functools.partial(expert_kernel, j),
        out_shape=(
            jax.ShapeDtypeStruct((groups, cap, dim), BF),
            jax.ShapeDtypeStruct((groups, cap, dim), BF),
            jax.ShapeDtypeStruct((groups, cap, LANES), F32),
            jax.ShapeDtypeStruct((groups, slices, kinds, depth, depth), BF),
        ),
        grid_spec=pltpu.PrefetchScalarGridSpec(
            num_scalar_prefetch=6,
            grid=(steps[0].shape[0],),
            in_specs=[
                pl.BlockSpec((1, TILE, dim), row_map),
                pl.BlockSpec((1, TILE, dim), row_map),
                pl.BlockSpec((1, TILE, LANES), row_map),
            ] + [ANY] * (3 + slices),
            out_specs=[
                pl.BlockSpec((1, TILE, dim), out_map),
                pl.BlockSpec((1, TILE, dim), out_map),
                pl.BlockSpec((1, TILE, LANES), out_map),
                pl.BlockSpec((1, slices, kinds, depth, depth), lambda k, zs, ts, at, *_: (at[k], 0, 0, 0, 0)),
            ],
            scratch_shapes=[
                pltpu.VMEM((4, dim, depth), F32),
                pltpu.VMEM((2, depth, dim), F32),
                pltpu.VMEM((2, slices, kinds, depth, depth), BF),
                pltpu.SemaphoreType.DMA((2, slices, kinds + 1)),
            ],
        ),
        compiler_params=pltpu.CompilerParams(
            dimension_semantics=("arbitrary",), vmem_limit_bytes=56 << 20
        ),
        cost_estimate=pl.CostEstimate(
            flops=18 * groups * 4 * TILE * dim * ff, bytes_accessed=groups * 4 * TILE * dim * 8, transcendentals=0
        ),
    )(*steps[:4], offs, steps[4], hs, dys, wr, *own, *remote)


def combine_kernel(experts, n_local, cnt, start, limit, rank_ref, w_ref, *refs):
    outs, dhs, dws = refs[:n_local], refs[n_local:2 * n_local], refs[2 * n_local:3 * n_local]
    y_ref, dn_ref, dk_ref, obuf, dbuf, kbuf, sel, one, spread, ox, dx, kx, sem, xsem = refs[3 * n_local:]
    i = pl.program_id(0)
    n = pl.num_programs(0)
    slot = lax.rem(i, 2)
    lane = lax.broadcasted_iota(jnp.int32, (CHUNK, LANES), 1)
    row_lane = lax.broadcasted_iota(jnp.int32, (SEG, LANES), 1)

    def copies(step, s, e):
        z, j = divmod(e, n_local)
        at = pl.multiple_of(start[step * experts + e], ALIGN)
        return (
            pltpu.make_async_copy(outs[j].at[z, pl.ds(at, SEG)], obuf.at[s, pl.ds(e * SEG, SEG)], sem.at[s, 0, e]),
            pltpu.make_async_copy(dhs[j].at[z, pl.ds(at, SEG)], dbuf.at[s, pl.ds(e * SEG, SEG)], sem.at[s, 1, e]),
            pltpu.make_async_copy(dws[j].at[z, pl.ds(at, SEG)], kbuf.at[s, pl.ds(e * SEG, SEG)], sem.at[s, 2, e]),
        )

    @pl.when(i == 0)
    def _():
        for e in range(experts):
            for cp in copies(0, 0, e):
                cp.start()

    @pl.when(i + 1 < n)
    def _():
        for e in range(experts):
            for cp in copies(i + 1, 1 - slot, e):
                cp.start()

    def split(v):
        hi = v.astype(BF).astype(F32)
        mid = (v - hi).astype(BF).astype(F32)
        low = v - hi - mid
        return hi, mid, low

    rank = rank_ref[...]
    w_parts = split(w_ref[...])
    for e in range(experts):
        same = lane == rank[:, e:e + 1]
        at = slice(e * SEG, (e + 1) * SEG)
        one[:, at] = jnp.where(same, 1.0, 0.0).astype(BF)
        for p in range(3):
            sel[p * CHUNK:(p + 1) * CHUNK, at] = jnp.where(same, w_parts[p][:, e:e + 1], 0.0).astype(BF)

    for e in range(experts):
        for cp in copies(i, slot, e):
            cp.wait()

    def spread_of(e, value):
        parts = split(value)
        out = jnp.where(row_lane == e, parts[0], 0.0)
        out = jnp.where(row_lane == experts + e, parts[1], out)
        return jnp.where(row_lane == 2 * experts + e, parts[2], out).astype(BF)

    for e in range(experts):
        at = pl.ds(e * SEG, SEG)
        spread[at, :] = spread_of(e, kbuf[slot, at, :])
    three = dot(sel[...], obuf[slot])
    y_ref[...] = three[:CHUNK] + three[CHUNK:2 * CHUNK] + three[2 * CHUNK:]
    dn_ref[...] = dot(one[...], dbuf[slot])
    dk_ref[...] = dot(one[...], spread[...])

    for e in range(experts):
        z, j = divmod(e, n_local)

        @pl.when(cnt[i * experts + e] > SEG)
        def _():
            base = start[i * experts + e]
            at = pl.multiple_of(jnp.minimum(base + SEG, limit[e] - SEG), ALIGN)
            extra = (
                pltpu.make_async_copy(outs[j].at[z, pl.ds(at, SEG)], ox, xsem.at[0]),
                pltpu.make_async_copy(dhs[j].at[z, pl.ds(at, SEG)], dx, xsem.at[1]),
                pltpu.make_async_copy(dws[j].at[z, pl.ds(at, SEG)], kx, xsem.at[2]),
            )
            for cp in extra:
                cp.start()
            for cp in extra:
                cp.wait()
            seen = rank_ref[:, e:e + 1]
            same = (lane + (at - base) == seen) & (seen >= SEG)
            pick = jnp.where(same, 1.0, 0.0).astype(BF)
            parts = split(w_ref[:, e:e + 1])
            for p in range(3):
                y_ref[...] += dot(jnp.where(same, parts[p], 0.0).astype(BF), ox[...])
            dn_ref[...] += dot(pick, dx[...])
            dk_ref[...] += dot(pick, spread_of(e, kx[...]))


def combine(tables, rank, w, outs, dhs, dws):
    tok = rank.shape[0]
    n_local = len(outs)
    groups, _, dim = outs[0].shape
    experts = groups * n_local
    n = tok // CHUNK
    return pl.pallas_call(
        functools.partial(combine_kernel, experts, n_local),
        out_shape=(
            jax.ShapeDtypeStruct((tok, dim), F32),
            jax.ShapeDtypeStruct((tok, dim), F32),
            jax.ShapeDtypeStruct((tok, LANES), F32),
        ),
        grid_spec=pltpu.PrefetchScalarGridSpec(
            num_scalar_prefetch=3,
            grid=(n,),
            in_specs=[
                pl.BlockSpec((CHUNK, experts), lambda i, *_: (i, 0)),
                pl.BlockSpec((CHUNK, experts), lambda i, *_: (i, 0)),
            ] + [ANY] * (3 * n_local),
            out_specs=[
                pl.BlockSpec((CHUNK, dim), lambda i, *_: (i, 0)),
                pl.BlockSpec((CHUNK, dim), lambda i, *_: (i, 0)),
                pl.BlockSpec((CHUNK, LANES), lambda i, *_: (i, 0)),
            ],
            scratch_shapes=[
                pltpu.VMEM((2, experts * SEG, dim), BF),
                pltpu.VMEM((2, experts * SEG, dim), BF),
                pltpu.VMEM((2, experts * SEG, LANES), F32),
                pltpu.VMEM((3 * CHUNK, experts * SEG), BF),
                pltpu.VMEM((CHUNK, experts * SEG), BF),
                pltpu.VMEM((experts * SEG, LANES), BF),
                pltpu.VMEM((SEG, dim), BF),
                pltpu.VMEM((SEG, dim), BF),
                pltpu.VMEM((SEG, LANES), F32),
                pltpu.SemaphoreType.DMA((2, 3, experts)),
                pltpu.SemaphoreType.DMA((3,)),
            ],
        ),
        compiler_params=pltpu.CompilerParams(
            dimension_semantics=("arbitrary",), vmem_limit_bytes=56 << 20
        ),
        cost_estimate=pl.CostEstimate(
            flops=8 * n * CHUNK * experts * SEG * dim, bytes_accessed=n * experts * SEG * dim * 4, transcendentals=0
        ),
        name="combine",
    )(*tables, rank, w, *outs, *dhs, *dws)


def small_sum_kernel(axes, sizes, whole_ref, split_ref, whole_out, split_out, got_w, got_s, mine, send, recv):
    n = math.prod(sizes)
    share = split_ref.shape[0] // n if split_ref is not None else 0
    me = 0
    for axis, size in zip(axes, sizes):
        me = me * size + lax.axis_index(axis)

    def place(p):
        out = []
        for size in reversed(sizes):
            out.append(lax.rem(p, size))
            p = p // size
        return dict(zip(axes, reversed(out)))

    barrier = pltpu.get_barrier_semaphore()
    for k in range(1, n):
        pl.semaphore_signal(barrier, inc=1, device_id=place(lax.rem(me + k, n)), device_id_type=pl.DeviceIdType.MESH)
    pl.semaphore_wait(barrier, n - 1)

    def copy(src, dst, what, k):
        peer = lax.rem(me + k, n)
        return pltpu.make_async_remote_copy(
            src_ref=src, dst_ref=dst, send_sem=send.at[what, k], recv_sem=recv.at[what, k],
            device_id=place(peer), device_id_type=pl.DeviceIdType.MESH,
        )

    def rows_of(p):
        return split_ref.at[pl.ds(pl.multiple_of(p * share, 8), share)]

    first = []
    for k in range(1, n):
        first.append(copy(whole_ref, got_w.at[me], 0, k))
        if split_ref is not None:
            first.append(copy(rows_of(lax.rem(me + k, n)), got_s.at[me], 1, k))
    for cp in first:
        cp.start()
    got_w[me] = whole_ref[...]
    if split_ref is not None:
        got_s[me] = split_ref[pl.ds(pl.multiple_of(me * share, 8), share)]
    for cp in first:
        cp.wait()
    whole_out[...] = jnp.sum(got_w[...], axis=0)
    if split_ref is not None:
        mine[...] = jnp.sum(got_s[...], axis=0)
        own = pl.ds(pl.multiple_of(me * share, 8), share)
        split_out[own, :] = mine[...]
        second = [copy(mine, split_out.at[own], 2, k) for k in range(1, n)]
        for cp in second:
            cp.start()
        for cp in second:
            cp.wait()


def small_sum(axes, sizes, ident, whole, split=None):
    n = math.prod(sizes)
    vmem = pl.BlockSpec(memory_space=pltpu.VMEM)
    scratch = [pltpu.VMEM((n,) + whole.shape, F32)]
    if split is not None:
        scratch += [pltpu.VMEM((n, split.shape[0] // n, LANES), F32), pltpu.VMEM((split.shape[0] // n, LANES), F32)]
    scratch += [pltpu.SemaphoreType.DMA((3, n)), pltpu.SemaphoreType.DMA((3, n))]
    kernel = functools.partial(small_sum_kernel, axes, sizes)
    if split is None:
        def body(w, wo, gw, ss, rs):
            kernel(w, None, wo, None, gw, None, None, ss, rs)

        args = (whole,)
    else:
        body = kernel
        args = (whole, split)
    out = pl.pallas_call(
        body,
        out_shape=tuple(jax.ShapeDtypeStruct(v.shape, F32) for v in args),
        in_specs=[vmem] * len(args),
        out_specs=tuple([vmem] * len(args)),
        scratch_shapes=scratch,
        compiler_params=pltpu.CompilerParams(collective_id=ident, has_side_effects=True),
    )(*args)
    return out


def assemble_kernel(first, offs, *refs):
    pieces, refs = refs[:4], refs[4:]
    gate, up, down, buf, sem_in, sem_out = refs[-6:]
    slices, count, _, block, _ = buf.shape
    experts = pl.ds(first, count)
    loads = [pltpu.make_async_copy(pieces[r], buf.at[r], sem_in.at[r]) for r in range(slices)]
    for cp in loads:
        cp.start()
    stores = []
    for r in range(slices):
        loads[r].wait()
        at = pl.ds(pl.multiple_of(offs[r] * block, block), block)
        for f in range(2):
            part = pl.ds(f * block, block)
            for t, target in enumerate((gate.at[experts, at, part], up.at[experts, at, part], down.at[experts, part, at])):
                cp = pltpu.make_async_copy(buf.at[r, :, 2 * t + f], target, sem_out.at[r, 2 * t + f])
                cp.start()
                stores.append(cp)
    for cp in stores:
        cp.wait()


def assemble(first, offs, pieces, shapes, prev=()):
    count, kinds, depth = pieces[0].shape[:3]
    slices = len(pieces)
    return pl.pallas_call(
        functools.partial(assemble_kernel, first),
        out_shape=tuple(jax.ShapeDtypeStruct(v, BF) for v in shapes),
        grid_spec=pltpu.PrefetchScalarGridSpec(
            num_scalar_prefetch=1,
            grid=(),
            in_specs=[ANY] * (slices + len(prev)),
            out_specs=[ANY] * 3,
            scratch_shapes=[
                pltpu.VMEM((slices, count, kinds, depth, depth), BF),
                pltpu.SemaphoreType.DMA((slices,)),
                pltpu.SemaphoreType.DMA((slices, kinds)),
            ],
        ),
        input_output_aliases={1 + slices + k: k for k in range(len(prev))},
        compiler_params=pltpu.CompilerParams(vmem_limit_bytes=24 << 20),
    )(offs, *pieces, *prev)


def finish_kernel(x_ref, near_ref, back_ref, *refs):
    refs[-1][...] = (x_ref[...].astype(F32) + (near_ref[...] + back_ref[...])).astype(BF)


def finish(part, x, near, back, prev=()):
    tok, dim = x.shape
    n = back.shape[0] // CHUNK
    at = pl.BlockSpec((CHUNK, dim), lambda i: (i + part * n, 0))
    return pl.pallas_call(
        finish_kernel,
        out_shape=jax.ShapeDtypeStruct((tok, dim), BF),
        grid=(n,),
        in_specs=[at, at, pl.BlockSpec((CHUNK, dim), lambda i: (i, 0))] + [ANY] * len(prev),
        out_specs=at,
        input_output_aliases={3: 0} if prev else {},
        cost_estimate=pl.CostEstimate(flops=2 * back.size, bytes_accessed=12 * back.size, transcendentals=0),
    )(x, near, back, *prev)


def layout_tables(mask):
    tok, experts = mask.shape
    n = tok // CHUNK
    m3 = mask.reshape(n, CHUNK, experts)
    before = jnp.tril(jnp.ones((CHUNK, CHUNK), BF), -1)
    rank = jnp.einsum('ts,cse->cte', before, m3.astype(BF), preferred_element_type=F32)
    rank = jnp.where(m3 > 0, rank, -1.0).astype(jnp.int32).reshape(tok, experts)
    cnt = jnp.sum(m3, axis=1).astype(jnp.int32)
    return rank, cnt


def expert_steps(tiles, z_at, most):
    groups, n_local = tiles.shape
    turned = sum(jnp.where(z_at == q, jnp.roll(tiles, -q, axis=0), 0) for q in range(groups))
    ends = jnp.cumsum(turned, axis=0)
    steps = jnp.arange(groups * most, dtype=jnp.int32)[:, None]
    item_z = jnp.minimum(sum((steps >= ends[None, z]).astype(jnp.int32) for z in range(groups)), groups - 1)
    first = sum(jnp.where(item_z == z, (ends - turned)[None, z], 0) for z in range(groups))
    item_t = jnp.minimum(steps, ends[-1:] - 1) - first
    item_at = lax.rem(item_z + z_at, groups)
    return [(item_z[:, j], item_t[:, j], item_at[:, j], turned[:, j], ends[-1, j:j + 1]) for j in range(n_local)]


def windows(tables, rank, limit):
    experts = limit.shape[0]
    cnt, start = tables[0].reshape(-1, experts), tables[1].reshape(-1, experts)
    at = jnp.minimum(start, limit[None, :] - SEG)
    shift = start - at
    rank = rank.reshape(-1, CHUNK, experts)
    rank = jnp.where(rank >= 0, rank + shift[:, None, :], -1).reshape(-1, experts)
    return ((cnt + shift).reshape(-1), at.reshape(-1), limit), rank


def solution(mesh):
    ep_size = mesh.shape['ep']
    dp_size = mesh.shape['dp']
    n_dev = ep_size * dp_size
    nz, ny = ep_size // 2, 2
    fine = Mesh(mesh.devices.reshape(nz, ny, dp_size), ('z', 'y', 'b'))
    row_spec = P(('z', 'y', 'b'), None)
    exp_spec = P(('z', 'y'), None, None)
    swap = [(0, 1), (1, 0)]
    to_x = [(q, q ^ 2) for q in range(dp_size)]
    to_core = [(q, q ^ 1) for q in range(dp_size)]

    def spread_slices(own):
        other_x = send(own, 'b', to_x)
        return (own, send(own, 'b', to_core), other_x, send(other_x, 'b', to_core))

    def send(v, axis, pairs):
        return lax.ppermute(v, axis, pairs)

    def block_of(hidden_in, topk_idx, grad_out, norm_gain, w_router, w_gate, w_up, w_down):
        tok, dim = hidden_in.shape
        experts = w_router.shape[1]
        top_k = topk_idx.shape[1]
        n_local, _, _ = w_gate.shape
        tok_total = tok * n_dev
        mine = nz * n_local
        chunks = tok // CHUNK
        per_dev = tok * top_k // experts + tok * top_k // (2 * experts)
        cap = -(-(2 * per_dev + 2 * chunks * (ALIGN - 1)) // TILE) * TILE + TILE
        depth = dim // dp_size
        z_at = lax.axis_index('z')
        y_at = lax.axis_index('y')
        b_at = lax.axis_index('b')
        offs = jnp.bitwise_xor(b_at, jnp.arange(dp_size, dtype=jnp.int32))

        part = tok // FAR_PARTS
        dy_far = send(grad_out, 'y', swap)

        offers = offer(b_at.reshape(1), w_gate, w_up, w_down, depth)
        pieces = []
        for j in range(n_local):
            gathered = lax.all_gather(offers[j], 'z')
            pieces.append(spread_slices(others_of(z_at.reshape(1), gathered)))

        x_f = hidden_in.astype(F32)
        inv_rms = lax.rsqrt(jnp.mean(x_f * x_f, axis=-1, keepdims=True) + EPS)
        normed = (x_f * inv_rms * norm_gain).astype(BF)
        h_far = [send(normed[p * part:(p + 1) * part], 'y', swap) for p in range(FAR_PARTS)]
        logits = jnp.dot(normed, w_router, preferred_element_type=F32)
        probs = jax.nn.softmax(logits, axis=-1)
        eye = jnp.arange(experts, dtype=jnp.int32)
        mask = jnp.zeros((tok, experts), F32)
        for k in range(top_k):
            mask = mask + (topk_idx[:, k:k + 1] == eye[None, :]).astype(F32)
        chosen = mask * probs
        chosen_sum = jnp.sum(chosen, axis=1, keepdims=True)
        weights = chosen / chosen_sum

        def halves(v):
            v4 = v.reshape(tok, nz, ny, n_local)
            a, b = v4[:, :, 0].reshape(tok, mine), v4[:, :, 1].reshape(tok, mine)
            own = jnp.where(y_at == 0, a, b)
            return own, jnp.where(y_at == 0, b, a)

        m_near, m_send = halves(mask)
        w_near, w_send = halves(weights)
        stats_own = jnp.pad(jnp.stack([jnp.sum(mask, axis=0), jnp.sum(probs, axis=0)]), ((0, 6), (0, 0)))
        far = send(jnp.concatenate([jnp.concatenate([m_send, w_send], axis=1), stats_own], axis=0), 'y', swap)

        rank_near, cnt_near = layout_tables(m_near)
        pad_near = (cnt_near + ALIGN - 1) // ALIGN * ALIGN
        end_near = jnp.cumsum(pad_near, axis=0)
        near = (cnt_near.reshape(-1), (end_near - pad_near).reshape(-1), end_near[-1])

        rows = dispatch(0, False, near, normed, grad_out, rank_near.T, w_near.T, cap)

        far, marks = lax.optimization_barrier((far, rows[2]))
        rows = (rows[0], rows[1], marks)
        m_far, w_far, stats_far = far[:tok, :mine], far[:tok, mine:], far[tok:]
        rank_far, cnt_far = layout_tables(m_far)
        pad_far = (cnt_far + ALIGN - 1) // ALIGN * ALIGN
        end_far = jnp.cumsum(pad_far, axis=0) + end_near[-1]
        end = end_far[-1]
        far_t = (cnt_far.reshape(-1), (end_far - pad_far).reshape(-1), end)
        used = ((end + TILE - 1) // TILE).reshape(nz, n_local)
        limit = used.reshape(-1) * TILE
        steps = expert_steps(used, z_at, cap // TILE - 1)

        def window_parts(tables, rank, w, parts):
            (c, at, lim), rank = windows(tables, rank, limit)
            n, m = c.shape[0] // parts, tok // parts
            return [
                ((c[p * n:(p + 1) * n], at[p * n:(p + 1) * n], lim), rank[p * m:(p + 1) * m], w[p * m:(p + 1) * m])
                for p in range(parts)
            ]

        far_windows = window_parts(far_t, rank_far, w_far, FAR_PARTS)
        near_windows = window_parts(near, rank_near, w_near, 1)
        far_rank, far_w = rank_far.T, w_far.T
        far_t, far_rank, far_w, steps, far_windows, near_windows = lax.optimization_barrier(
            (far_t, far_rank, far_w, steps, far_windows, near_windows)
        )
        for p in range(FAR_PARTS):
            n = far_t[0].shape[0] // FAR_PARTS
            table = (far_t[0][p * n:(p + 1) * n], far_t[1][p * n:(p + 1) * n], far_t[2])
            at_p = slice(p * part, (p + 1) * part)
            rows = dispatch(
                1 + p, p == FAR_PARTS - 1, table, h_far[p], dy_far, far_rank[:, at_p], far_w[:, at_p], cap, rows
            )

        outs, dhs, dws, sums = [], [], [], []
        for j in range(n_local):
            o, dh, dw, gw = run_experts(j, n_local, steps[j], offs, *rows, (w_gate, w_up, w_down), pieces[j])
            steps, dw = lax.optimization_barrier((steps, dw))
            outs.append(o)
            dhs.append(dh)
            dws.append(dw)
            if j < n_local - 1:
                sums.append(lax.psum_scatter(gw.reshape((nz * dp_size,) + gw.shape[2:]), ('z', 'b'), scatter_dimension=0))

        def total(v):
            return v[:, :mine] + v[:, mine:2 * mine] + v[:, 2 * mine:3 * mine]

        returned, ties = [], []
        for args in far_windows:
            y_far, dn_far, dk_far = combine(*args, outs, dhs, dws)
            ties.append(dk_far)
            returned.append((send(total(dk_far), 'y', swap), send(dn_far, 'y', swap), send(y_far, 'y', swap)))
        stats_in = jnp.pad(stats_own + stats_far, ((0, 0), (0, LANES - experts)))
        gw, stats_in, *_ = lax.optimization_barrier((gw, stats_in, *ties))
        (stats,) = small_sum(('z', 'b'), (nz, dp_size), 0, stats_in)
        gw, stats = lax.optimization_barrier((gw, stats))
        slice_of = [lax.dynamic_index_in_dim(gw, offs[r], 1, keepdims=False) for r in range(dp_size)]
        core_own = send(slice_of[1], 'b', to_core)
        core_x = send(slice_of[3], 'b', to_core)
        for_x = (slice_of[2].astype(F32) + core_x.astype(F32)).astype(BF)
        from_x = send(for_x, 'b', to_x)
        mine_sum = slice_of[0].astype(F32) + core_own.astype(F32) + from_x.astype(F32)
        sums.append(lax.psum_scatter(mine_sum.astype(BF), 'z', scatter_dimension=0))
        dk_back, dn_back = (jnp.concatenate([v[q] for v in returned], axis=0) for q in range(2))
        y_back = [v[2] for v in returned]
        y_near, dn_near, dk_near = combine(*near_windows[0], outs, dhs, dws)

        load_frac = stats[0, :experts] / (top_k * tok_total)
        aux_loss = ALPHA * experts * jnp.sum(load_frac * stats[1, :experts] / tok_total)
        near4 = total(dk_near).reshape(tok, nz, n_local)
        back4 = dk_back.reshape(tok, nz, n_local)
        d_weight = jnp.stack([jnp.where(y_at == 0, near4, back4), jnp.where(y_at == 0, back4, near4)], axis=2).reshape(tok, experts)
        d_chosen = (d_weight - jnp.sum(weights * d_weight, axis=1, keepdims=True)) / chosen_sum
        aux_coef = AUX_SCALE * math.sqrt(dim * experts) * experts
        d_prob = mask * d_chosen + aux_coef * load_frac[None, :]
        d_logit = probs * (d_prob - jnp.sum(probs * d_prob, axis=1, keepdims=True))
        d_logit_bf = d_logit.astype(BF)
        router_part = jnp.einsum('td,te->de', normed, d_logit_bf, preferred_element_type=F32)
        d_normed = dn_near + dn_back + jnp.einsum('te,de->td', d_logit_bf, w_router, preferred_element_type=F32)
        gain_part = jnp.sum(d_normed * x_f * inv_rms, axis=0)
        d_scaled = d_normed * norm_gain
        inv_cube = inv_rms * inv_rms * inv_rms
        grad_in = (grad_out.astype(F32) + inv_rms * d_scaled - x_f * inv_cube * jnp.mean(d_scaled * x_f, axis=-1, keepdims=True)).astype(BF)
        sums_yz = small_sum(('z', 'b'), (nz, dp_size), 1, gain_part.reshape(-1, LANES), router_part.reshape(-1, LANES))
        both = jnp.concatenate(sums_yz, axis=0)
        both = both + send(both, 'y', swap)
        gain_rows = dim // LANES

        *early, grad_in, _ = lax.optimization_barrier((*sums[:-1], grad_in, sums_yz[0]))
        late, grad_in = lax.optimization_barrier((sums[-1], grad_in))
        shapes = (w_gate.shape, w_up.shape, w_down.shape)
        grads = assemble(0, offs, spread_slices(jnp.stack(early)), shapes)
        grads = assemble(n_local - 1, offs, spread_slices(late[None]), shapes, grads)
        block_out = ()
        for p in range(FAR_PARTS):
            block_out = (finish(p, hidden_in, y_near, y_back[p], block_out),)
        block_out = block_out[0]
        return (block_out, grad_in, aux_loss, both[:gain_rows].reshape(dim), both[gain_rows:].reshape(dim, experts), *grads)


    return jax.shard_map(
        block_of,
        mesh=fine,
        in_specs=(row_spec, row_spec, row_spec, P(None), P(None, None), exp_spec, exp_spec, exp_spec),
        out_specs=(row_spec, row_spec, P(), P(None), P(None, None), exp_spec, exp_spec, exp_spec),
        check_vma=False,
    )
```
